32 devices in a mesh: groups: 2 (over x), ep: 8 (over z, y), section: 2 (over core).
Axes of the slice: x: 2, y: 2, z: 4, core: 2. Of those that a mesh axis runs over, the one named last changes fastest.
Arguments:
- resid: bfloat16 [2048, 4096], P(('groups', 'ep')), parts along dimension 0, may hold values from -6 to 6
- norm_gain: bfloat16 [4096], replicated, may hold values from 0.3984375 to 1.59375
- gate_logits: float32 [2048, 8], P(('groups', 'ep')), parts along dimension 0, may hold values from 0.1 to 1
- routes: int32 [2048, 8], P(('groups', 'ep')), parts along dimension 0, may hold values from 0 to 31, all different within a row; in each aligned block of 128 rows (0 to 127, 128 to 255, ...) at most 40 rows name the same one
- w_gate: bfloat16 [32, 4096, 768], P('ep', None, 'section'), may hold values from -0.09375 to 0.09375
- w_up: bfloat16 [32, 4096, 768], P('ep', None, 'section'), may hold values from -0.09375 to 0.09375
- w_down: bfloat16 [32, 768, 4096], P('ep', 'section'), may hold values from -0.21875 to 0.21875
- keys_raw: bfloat16 [2048, 512], P(('groups', 'ep'), 'section'), parts along dimension 0, may hold values from -6 to 6
- values_raw: bfloat16 [2048, 512], P(('groups', 'ep'), 'section'), parts along dimension 0, may hold values from -6 to 6
- k_gain: bfloat16 [128], replicated, may hold values from 0.25 to 1.75
- lengths: int32 [16], P(('groups', 'ep')), parts along dimension 0, may hold values from 32 to 128
- page_owner: int32 [16, 8], P(('groups', 'ep')), parts along dimension 0, may hold values from 0 to 7, as said below
- page_slot: int32 [16, 8], P(('groups', 'ep')), parts along dimension 0, may hold values from 0 to 7, as said below
Outputs:
- moe_out: bfloat16 [2048, 4096], P(('groups', 'ep'), 'section'), parts along dimension 0
- kv_cache: bfloat16 [128, 16, 2, 512], P(('groups', 'ep'), None, None, 'section'), parts along dimension 0
The draws below stay inside these ranges and needn't reach their ends.
There are 2 independent parts, one for each index of `groups`. The reference program is written for one: setup_inputs(seed, part) draws one part's arguments, and reference() takes and returns one part's arrays. A program takes and returns all parts, laid end to end along the dimension named above; an argument that names none is the same for every part. Nothing has to cross between parts.
Inputs may be any that keep to these rules, and one draw needn't show every extreme that they name: `page_owner`: each prompt sends its 8 pages to 4 different owners, exactly 2 pages to each of them; every owner receives exactly 8 pages. `page_slot`: the pages that reach one owner have different slots, so every slot of every owner is filled once.
All inputs are finite; a program needn't handle non-finite values.
Results may differ from the reference program's by a relative error of at most 0.0076.
Values may be sent and summed in bfloat16 or wider, within the bound.
A program may use at most 128 MiB of HBM per device.

```python
import math
import jax
import jax.numpy as jnp
import numpy as np
from jax import lax

D = 4096
HEAD = 128
KV_HEADS = 4
TOP = 8
FF = 768
EXPERTS = 32
TOK_DEV = 128
PAGE = 16
CAP = 40
PAGES = 8
SEQS = 8
TOKENS = 1024


def page_plan(key):
    base = jax.random.fold_in(key, 4242)
    streams = jax.random.split(base, 5)
    owner_order = jax.random.permutation(streams[0], SEQS)
    source_order = jax.random.permutation(streams[1], SEQS)
    shifts = jax.random.permutation(streams[2], SEQS)[:PAGES // 2]
    group_owner = owner_order[(source_order[:, None] + shifts[None, :]) % SEQS]
    column_perm = jax.vmap(lambda sub: jax.random.permutation(sub, PAGES))(jax.random.split(streams[3], SEQS))
    owner = jnp.take_along_axis(group_owner, column_perm // 2, axis=1)
    slot_perm = jax.vmap(lambda sub: jax.random.permutation(sub, PAGES))(jax.random.split(streams[4], SEQS))
    slot = slot_perm[owner, column_perm]
    return (owner.astype(jnp.int32), slot.astype(jnp.int32))


def draw_page_owner(key, part):
    return page_plan(key)[0]


def draw_page_slot(key, part):
    return page_plan(key)[1]


def plant(values, stream_key, least, largest):
    spot = [jax.random.randint(jax.random.fold_in(stream_key, axis), (), 0, length) for axis, length in enumerate(values.shape)]
    longest = values.shape.index(max(values.shape))
    beside = spot[:longest] + [(spot[longest] + 1) % values.shape[longest]] + spot[longest + 1:]
    return values.at[tuple(spot)].set(least).at[tuple(beside)].set(largest)


def level_of(key, shape, shards, low, top_value):
    def one(dim, parts):
        steps = jax.random.uniform(jax.random.fold_in(jax.random.fold_in(key, 6), dim), (parts,), jnp.float32, low / len(shards), top_value / len(shards))
        return jnp.repeat(jnp.exp(steps), shape[dim] // parts).reshape((-1,) + (1,) * (len(shape) - dim - 1))

    level = one(*shards[0])
    for cut in shards[1:]:
        level = level * one(*cut)
    return level


def deal_out(stream_key, own, number, rows, number_of, top, limit, slope):
    sequence = jax.random.permutation(stream_key, number_of)
    packed, ordinary = shares(number_of, rows * top, limit, slope, True), shares(number_of, rows * top, limit, slope, False)
    places = jnp.arange(number_of)

    def named(sizes, offset_by):
        used = int((sizes > 0).sum())
        fixed = max(1, used // 4)
        moved = fixed + (places - fixed + offset_by * (used - fixed)) % max(1, number_of - fixed)
        return jnp.zeros((number_of,), jnp.int32).at[sequence[jnp.where(places < fixed, places, moved)]].set(jnp.asarray(sizes, jnp.int32))

    sizes = jnp.where(number % 4 == 0, named(packed, number // 4), named(ordinary, number - number // 4 - 1))
    mixed = jax.random.permutation(jax.random.fold_in(own, 3), number_of)
    source_of, sink = mixed[0:number_of // 2 * 2:2], mixed[1:number_of // 2 * 2:2]
    room = jnp.minimum(sizes[source_of] - 1, limit - sizes[sink]) // 2
    room = jnp.where((source_of == sequence[0]) | (sink == sequence[0]) | (sizes[sink] == 0), 0, jnp.maximum(room, 0))
    moved = jax.random.randint(jax.random.fold_in(own, 4), (number_of // 2,), 0, 1 << 20) % (room + 1)
    sizes = sizes.at[source_of].add(-moved).at[sink].add(moved)
    labels = jnp.searchsorted(jnp.cumsum(sizes), jnp.arange(rows * top), side="right").astype(jnp.int32)
    listing = labels.reshape(top, rows).T
    listing = listing[jax.random.permutation(jax.random.fold_in(own, 1), rows)]
    offset_by = jax.random.randint(jax.random.fold_in(own, 2), (rows, 1), 0, top)
    return jnp.take_along_axis(listing, (jnp.arange(top)[None, :] + offset_by) % top, axis=1)


def shares(number_of, total, limit, skew, full):
    loads = [(1 << 20) // math.isqrt(grade ** skew) + 1 for grade in range(1, number_of + 1)]
    largest = limit if full else min(limit, max(-(-total // number_of), total * loads[0] // sum(loads)))
    least = 1 if total - largest >= number_of - 1 else 0
    holding, spare = [largest] + [least] * (number_of - 1), total - largest - least * (number_of - 1)
    while spare > 0:
        movable = [i for i in range(1, number_of) if holding[i] < largest] or [i for i in range(1, number_of) if holding[i] < limit]
        pool, budget = sum([loads[i] for i in movable]), spare
        for i in movable:
            more = min(limit - holding[i], max(1, budget * loads[i] // pool), spare)
            holding[i] = holding[i] + more
            spare = spare - more
    return np.array(holding)


def noise(stream_key, shape, spread, bound, shards=(), kind=jnp.bfloat16):
    array = spread * jax.random.normal(stream_key, shape, jnp.float32)
    if shards:
        array = array * level_of(stream_key, shape, shards, -0.22, 0.18)
    return jnp.clip(array, -bound, bound).astype(kind)


def setup_inputs(seed: int = 0, part: int = 0) -> dict:
    arg_keys = jax.random.split(jax.random.key(seed), 14)
    part_keys = jax.random.split(jax.random.fold_in(arg_keys[13], part), 14)
    resid = noise(part_keys[0], (TOKENS, D), 1.0, 6.0, ((0, 8),))
    norm_gain = jnp.clip(1.0 + 0.12 * jax.random.normal(arg_keys[1], (D,), jnp.float32), 0.3984375, 1.59375).astype(jnp.bfloat16)
    gate_logits = jnp.clip(jnp.exp(math.log(1.0) - 2.3025851 * jax.random.uniform(part_keys[2], (TOKENS, TOP), jnp.float32) ** level_of(part_keys[2], (TOKENS, TOP), ((0, 8),), -0.2, 0.2)), 0.1, 1.0)
    routes_keys = jax.random.split(jax.random.fold_in(part_keys[3], 1), TOKENS // TOK_DEV)
    routes_turns = jax.random.permutation(jax.random.fold_in(part_keys[3], 3), TOKENS // TOK_DEV)
    routes = jax.vmap(lambda own, number: deal_out(jax.random.fold_in(part_keys[3], 2), own, number, TOK_DEV, EXPERTS, TOP, CAP, 1))(routes_keys, routes_turns).reshape((TOKENS, TOP))
    w_gate = noise(arg_keys[4], (EXPERTS, D, FF), D ** -0.5, 0.09375, ((0, 8), (2, 2)))
    w_up = noise(arg_keys[5], (EXPERTS, D, FF), D ** -0.5, 0.09375, ((0, 8), (2, 2)))
    w_down = noise(arg_keys[6], (EXPERTS, FF, D), FF ** -0.5, 0.21875, ((0, 8), (1, 2)))
    keys_raw = noise(part_keys[7], (TOKENS, KV_HEADS * HEAD), 1.0, 6.0, ((0, 8), (1, 2)))
    values_raw = noise(part_keys[8], (TOKENS, KV_HEADS * HEAD), 1.0, 6.0, ((0, 8), (1, 2)))
    k_gain = jnp.clip(1.0 + 0.15 * jax.random.normal(arg_keys[9], (HEAD,), jnp.float32), 0.25, 1.75).astype(jnp.bfloat16)
    lengths = plant(jax.random.randint(part_keys[10], (SEQS,), TOK_DEV // 4, TOK_DEV + 1), jax.random.fold_in(part_keys[10], 1), TOK_DEV // 4, TOK_DEV).astype(jnp.int32)
    page_owner = draw_page_owner(jax.random.fold_in(jax.random.fold_in(arg_keys[13], part), 71), part)
    page_slot = draw_page_slot(jax.random.fold_in(jax.random.fold_in(arg_keys[13], part), 71), part)
    return {"resid": resid, "norm_gain": norm_gain, "gate_logits": gate_logits, "routes": routes, "w_gate": w_gate, "w_up": w_up, "w_down": w_down, "keys_raw": keys_raw, "values_raw": values_raw, "k_gain": k_gain, "lengths": lengths, "page_owner": page_owner, "page_slot": page_slot}


def rms_scale(values, gain_row):
    mean_square = lax.optimization_barrier(jnp.mean(values * values, axis=-1, keepdims=True))
    return values * lax.rsqrt(mean_square + 1e-06) * gain_row

def rotate_keys(key_block, position):
    half_size = key_block.shape[-1] // 2
    frequency = jnp.exp(jnp.arange(half_size, dtype=jnp.float32) * (-2.0 / key_block.shape[-1]) * math.log(1000000.0))
    angles = position.astype(jnp.float32)[:, None, None] * frequency
    cosine = jnp.cos(angles)
    sine_part = jnp.sin(angles)
    first_half = key_block[..., :half_size]
    second = key_block[..., half_size:]
    return jnp.concatenate([first_half * cosine - second * sine_part, second * cosine + first_half * sine_part], axis=-1)

def reference(resid, norm_gain, gate_logits, routes, w_gate, w_up, w_down, keys_raw, values_raw, k_gain, lengths, page_owner, page_slot):
    total_tokens = SEQS * TOK_DEV
    token_ids = jnp.arange(total_tokens, dtype=jnp.int32)
    position = token_ids % TOK_DEV
    prompt_ids = token_ids // TOK_DEV
    is_live = position < lengths[prompt_ids]
    hidden = rms_scale(resid.astype(jnp.float32), norm_gain.astype(jnp.float32)).astype(jnp.bfloat16)
    logits = gate_logits.astype(jnp.float32)
    mixing = (logits / lax.optimization_barrier(jnp.sum(logits, axis=-1, keepdims=True))).astype(jnp.bfloat16)
    pair_count = TOK_DEV * TOP
    chosen = routes.reshape(SEQS, pair_count).astype(jnp.int32)
    live_rows = jnp.repeat(is_live, TOP).reshape(SEQS, pair_count)
    expert_hits = ((chosen[:, :, None] == jnp.arange(EXPERTS, dtype=jnp.int32)[None, None, :]) & live_rows[:, :, None]).astype(jnp.int32)
    slot_rank = lax.optimization_barrier(jnp.sum((jnp.cumsum(expert_hits, axis=1) - expert_hits) * expert_hits, axis=2))
    slot_span = SEQS * CAP
    dead_slot = EXPERTS * slot_span
    target = jnp.where(live_rows, chosen * slot_span + jnp.arange(SEQS, dtype=jnp.int32)[:, None] * CAP + slot_rank, dead_slot).astype(jnp.int32)
    row_token = jnp.repeat(token_ids, TOP).reshape(SEQS, pair_count)
    table = jnp.full((dead_slot + 1,), total_tokens, jnp.int32).at[target.reshape(-1)].set(row_token.reshape(-1))
    table = table[:dead_slot].reshape(EXPERTS, slot_span)
    padded = jnp.concatenate([hidden, jnp.zeros((1, D), jnp.bfloat16)], axis=0)

    def one_expert(expert_index):
        gathered = padded[table[expert_index]]
        gate_part = jnp.dot(gathered, w_gate[expert_index], preferred_element_type=jnp.float32)
        up_part = jnp.dot(gathered, w_up[expert_index], preferred_element_type=jnp.float32)
        active = (jax.nn.silu(gate_part) * up_part).astype(jnp.bfloat16)
        return jnp.dot(active, w_down[expert_index], preferred_element_type=jnp.float32).astype(jnp.bfloat16)
    expert_out = lax.map(one_expert, jnp.arange(EXPERTS, dtype=jnp.int32))
    flat_out = jnp.concatenate([expert_out.reshape(dead_slot, D), jnp.zeros((1, D), jnp.bfloat16)], axis=0)
    pair_slot = target.reshape(total_tokens, TOP)
    mixed = jnp.zeros((total_tokens, D), jnp.float32)
    for pick_index in range(TOP):
        mixed = mixed + mixing[:, pick_index].astype(jnp.float32)[:, None] * flat_out[pair_slot[:, pick_index]].astype(jnp.float32)
    moe_out = mixed.astype(jnp.bfloat16)
    head_rows = keys_raw.astype(jnp.float32).reshape(total_tokens, KV_HEADS, HEAD)
    normed = rms_scale(head_rows, k_gain.astype(jnp.float32))
    turned = rotate_keys(normed, position)
    key_rows = jnp.where(is_live[:, None, None], turned, 0.0).astype(jnp.bfloat16).reshape(total_tokens, KV_HEADS * HEAD)
    value_rows = jnp.where(is_live[:, None], values_raw, jnp.zeros_like(values_raw))
    stacked = jnp.stack([key_rows, value_rows], axis=1).reshape(SEQS * PAGES, PAGE, 2, KV_HEADS * HEAD)
    destination = (page_owner.astype(jnp.int32) * PAGES + page_slot.astype(jnp.int32)).reshape(-1)
    kv_cache = jnp.zeros_like(stacked).at[destination].set(stacked)
    return (moe_out, kv_cache)
```

```python
import functools
import math

import jax
import jax.numpy as jnp
import numpy as np
from jax import lax
from jax.experimental import pallas as pl
from jax.experimental.pallas import tpu as pltpu
from jax.sharding import PartitionSpec as P

PAGE = 16
CAP = 40
PER_OWNER = 2
F32 = jnp.float32
BF16 = jnp.bfloat16
MESH = pl.DeviceIdType.MESH
LIMIT = 67000000


def place(outer, inner):
    ep = lax.axis_index("ep")
    return ep, lax.axis_index("section"), lax.div(ep, inner), lax.rem(ep, inner)


def near_column(outer, z, i):
    low = jnp.where(2 * z < outer, z, outer - 1 - z)
    step = (i + 1) // 2
    both = jnp.where(i % 2 == 1, step, -step)
    offset = jnp.where(i <= 2 * low, both, i - low)
    return jnp.where(2 * z < outer, z + offset, z - offset)


def sides(outer, z, d, body):
    for side in (-1, 1):
        zz = z + side * d
        pl.when((zz >= 0) & (zz < outer))(functools.partial(body, side, zz))


def nt_dot(a, b):
    return lax.dot_general(a, b, (((1,), (1,)), ((), ())), preferred_element_type=F32)


def slot_match(meta, first, experts, slots, inner):
    rows = []
    tok = meta[0].shape[1]
    slot = lax.broadcasted_iota(jnp.int32, (slots, tok), 0).astype(F32)
    for j in range(experts):
        parts = []
        for p in range(inner):
            rank = meta[p][first + j : first + j + 1, :]
            goal = jnp.where(rank >= 0.0, rank + float(p * CAP), -1.0)
            parts.append(slot == goal)
        rows.append(parts)
    return rows


def experts_kernel(
    outer, inner, halves, chunks,
    resid, gain, routes, gates, length, keys, values, kgain, cosine, sine, owner, page_slot, wg, wu,
    act, metas, kv,
    rows, hidden, arrived, wbuf, pick, msend_buf, kvsend, kvrecv,
    send, recv, msend, mrecv, ksend, krecv, local, wsem,
):
    ep, core, z, y = place(outer, inner)
    peers = outer * inner
    tok, width = resid.shape
    cols = width // halves
    experts, _, ff = wg.shape
    slots = act.shape[2]
    piece = tok // chunks
    sib_kind = 1 + inner
    meta_rows = metas.shape[1]
    pages = owner.shape[1]
    kvw = keys.shape[1]

    def own_copy(h):
        return pltpu.make_async_copy(
            resid.at[:, pl.ds(h * cols, cols)], rows.at[ep, h], local.at[h]
        )

    def w_copy(j, which):
        return pltpu.make_async_copy(
            (wg, wu)[which].at[j], wbuf.at[j, :, pl.ds(which * ff, ff)], wsem.at[which, j]
        )

    for h in range(halves):
        own_copy(h).start()

    barrier = pltpu.get_barrier_semaphore()
    for k in range(1, peers):
        pl.semaphore_signal(
            barrier, inc=1, device_id={"ep": lax.rem(ep + k, peers), "section": core},
            device_id_type=MESH,
        )
    for k in range(1, halves):
        pl.semaphore_signal(
            barrier, inc=1, device_id={"ep": ep, "section": lax.rem(core + k, halves)},
            device_id_type=MESH,
        )
    for j in range(experts):
        for which in range(2):
            w_copy(j, which).start()
    for h in range(halves):
        own_copy(h).wait()
    pl.semaphore_wait(barrier, peers - 1 + halves - 1)

    def chunk_copy(block, half, k, kind, to_ep, to_core):
        at = (block, half, pl.ds(k * piece, piece), slice(None))
        return pltpu.make_async_remote_copy(
            src_ref=rows.at[at],
            dst_ref=rows.at[at],
            send_sem=send.at[kind, block],
            recv_sem=recv.at[block, half, k],
            device_id={"ep": to_ep, "section": to_core},
            device_id_type=MESH,
        )

    def block_sent(block, kind):
        pltpu.make_async_remote_copy(
            src_ref=rows.at[block, core],
            dst_ref=rows.at[block, core],
            send_sem=send.at[kind, block],
            recv_sem=recv.at[block, core, 0],
            device_id={"ep": ep, "section": lax.rem(core + 1, halves)},
            device_id_type=MESH,
        ).wait_send()

    def landed(block, half, k):
        chunk_copy(block, half, k, 0, ep, lax.rem(core + 1, halves)).wait_recv()

    def to_down(block, k):
        chunk_copy(block, core, k, 0, ep - inner, core).start()

    def to_up(block, k):
        chunk_copy(block, core, k, 1, ep + inner, core).start()

    def to_across(block, k):
        for n in range(1, inner):
            chunk_copy(block, core, k, 1 + n, z * inner + lax.rem(y + n, inner), core).start()

    def to_sibling(block, k):
        for n in range(1, halves):
            chunk_copy(
                block, core, k, sib_kind + n - 1, ep, lax.rem(core + n, halves)
            ).start()

    for k in range(chunks):
        pl.when(z > 0)(functools.partial(to_down, ep, k))
        pl.when(z < outer - 1)(functools.partial(to_up, ep, k))
        to_across(ep, k)

    number = experts * peers
    lane = lax.broadcasted_iota(jnp.int32, (1, tok), 1)
    live = lane.astype(F32) < length[...].astype(F32)
    mixing = gates[...] / jnp.sum(gates[...], axis=-1, keepdims=True)
    mixing = mixing.astype(BF16).astype(F32).T
    chosen = routes[...].astype(F32).T
    expert_id = lax.broadcasted_iota(jnp.int32, (number, tok), 0).astype(F32)
    hits = jnp.zeros((number, tok), F32)
    weight = jnp.zeros((number, tok), F32)
    for k in range(chosen.shape[0]):
        same = (chosen[k : k + 1, :] == expert_id) & live
        hits = hits + jnp.where(same, 1.0, 0.0)
        weight = weight + jnp.where(same, mixing[k : k + 1, :], 0.0)
    row_id = lax.broadcasted_iota(jnp.int32, (tok, tok), 0)
    col_id = lax.broadcasted_iota(jnp.int32, (tok, tok), 1)
    earlier = jnp.where(row_id < col_id, 1.0, 0.0).astype(BF16)
    rank = jnp.dot(hits.astype(BF16), earlier, preferred_element_type=F32)
    rank = jnp.where(hits > 0.0, rank, -1.0)

    own_t = jnp.zeros((1, tok), F32)
    slot_t = jnp.zeros((1, tok), F32)
    page_t = lax.div(lane, PAGE)
    for j in range(pages):
        own_t = jnp.where(page_t == j, owner[:, j : j + 1].astype(F32), own_t)
        slot_t = jnp.where(page_t == j, page_slot[:, j : j + 1].astype(F32), slot_t)
    own_here = jnp.broadcast_to(own_t, (tok, tok))
    before = (own_here.T == own_here) & (lax.div(row_id, PAGE) < lax.div(col_id, PAGE))
    order = jnp.sum(jnp.where(before, 1.0, 0.0), axis=0, keepdims=True) * (1.0 / PAGE)
    in_page = (lane - page_t * PAGE).astype(F32)
    key_t = (own_t * PER_OWNER + order) * PAGE + in_page
    goal_t = slot_t * PAGE + in_page
    pad_rows = jnp.zeros((meta_rows - 2 * experts - 2, tok), F32)
    for d in range(peers):
        mine = slice(d * experts, (d + 1) * experts)
        msend_buf[d] = jnp.concatenate([rank[mine], weight[mine], key_t, goal_t, pad_rows], axis=0)

    def meta_copy(n):
        to = lax.rem(ep + n, peers)
        return pltpu.make_async_remote_copy(
            src_ref=msend_buf.at[to],
            dst_ref=metas.at[ep],
            send_sem=msend.at[to],
            recv_sem=mrecv.at[ep],
            device_id={"ep": to, "section": core},
            device_id_type=MESH,
        )

    def kv_copy(n):
        to = lax.rem(ep + n, peers)
        return pltpu.make_async_remote_copy(
            src_ref=kvsend.at[to],
            dst_ref=kvrecv.at[ep],
            send_sem=ksend.at[to],
            recv_sem=krecv.at[ep],
            device_id={"ep": to, "section": core},
            device_id_type=MESH,
        )

    def from_peer(make, buf, sem, n):
        source = lax.rem(ep + n, peers)
        return pltpu.make_async_remote_copy(
            src_ref=buf.at[source],
            dst_ref=buf.at[source],
            send_sem=sem.at[source],
            recv_sem=make.at[source],
            device_id={"ep": source, "section": core},
            device_id_type=MESH,
        )

    for n in range(1, peers):
        meta_copy(n).start()
    metas[ep] = msend_buf[ep]

    live_c = lax.broadcasted_iota(jnp.int32, (tok, 1), 0).astype(F32) < length[...].astype(F32)
    head = kgain.shape[1]
    turned = []
    for h in range(kvw // head):
        x = keys[:, h * head : (h + 1) * head].astype(F32)
        x = x * lax.rsqrt(jnp.mean(x * x, axis=-1, keepdims=True) + 1e-06) * kgain[...].astype(F32)
        swapped = pltpu.roll(x, head // 2, 1)
        x = x * cosine[...] + swapped * sine[...]
        turned.append(jnp.where(live_c, x, 0.0).astype(BF16))
    turned.append(jnp.where(live_c, values[...].astype(F32), 0.0).astype(BF16))
    pairs = jnp.concatenate(turned, axis=1)
    piece_rows = PER_OWNER * PAGE
    group = 1
    while group * piece_rows < 256 and peers % (2 * group) == 0:
        group *= 2
    for d in range(0, peers, group):
        n = group * piece_rows
        want = (lax.broadcasted_iota(jnp.int32, (n, tok), 0) + d * piece_rows).astype(F32)
        chosen_rows = jnp.where(want == key_t, 1.0, 0.0).astype(BF16)
        out = jnp.dot(chosen_rows, pairs, preferred_element_type=F32).astype(BF16)
        for g in range(group):
            kvsend[d + g] = out[g * piece_rows : (g + 1) * piece_rows]
    for n in range(1, peers):
        kv_copy(n).start()
    kvrecv[ep] = kvsend[ep]

    def step(d):
        def body(k, carry):
            def one(side, zz):
                block = zz * inner + y
                landed(block, core, k)
                if side == 1:
                    pl.when(z > 0)(lambda: to_down(block, k))
                else:
                    pl.when(z < outer - 1)(lambda: to_up(block, k))
                to_across(block, k)
                to_sibling(block, k)

            sides(outer, z, d, one)
            return carry

        lax.fori_loop(0, chunks, body, 0)

    def across(zz):
        def body(k, carry):
            for n in range(1, inner):
                block = zz * inner + lax.rem(y + n, inner)
                landed(block, core, k)
                to_sibling(block, k)
            return carry

        lax.fori_loop(0, chunks, body, 0)

    tile = 512 if width % 512 == 0 else 128
    sub = 16

    def normalize(p, block):
        def body(i, carry):
            at = pl.ds(pl.multiple_of(i * sub, sub), sub)
            total = jnp.zeros((sub, 1), F32)
            for h in range(halves):
                for c in range(0, cols, tile):
                    x = rows[block, h, at, c : c + tile].astype(F32)
                    total = total + jnp.sum(x * x, axis=-1, keepdims=True)
            scale = lax.rsqrt(total * (1.0 / width) + 1e-06)
            to = pl.ds(pl.multiple_of(p * tok + i * sub, sub), sub)
            for h in range(halves):
                for c in range(0, cols, tile):
                    x = rows[block, h, at, c : c + tile].astype(F32)
                    g = gain[:, h * cols + c : h * cols + c + tile].astype(F32)
                    hidden[to, h * cols + c : h * cols + c + tile] = (x * scale * g).astype(BF16)
            return carry

        lax.fori_loop(0, tok // sub, body, 0)

    def compute(zz, own):
        for p in range(inner):
            block = zz * inner + p

            def wait_rest(block=block):
                for h in range(1, halves):
                    for k in range(chunks):
                        landed(block, lax.rem(core + h, halves), k)
                from_peer(mrecv, metas, msend, block - ep + peers).wait_recv()

            if own:
                pl.when(block != ep)(wait_rest)
            else:
                wait_rest()
            normalize(p, block)
        meta = [metas[zz * inner + p] for p in range(inner)]
        match = slot_match(meta, 0, experts, slots, inner)
        for j in range(experts):
            for p in range(inner):
                pick[j * slots : (j + 1) * slots, p * tok : (p + 1) * tok] = jnp.where(
                    match[j][p], 1.0, 0.0
                ).astype(BF16)

        def select(i, carry):
            at = pl.ds(pl.multiple_of(i * tile, tile), tile)
            arrived[:, at] = jnp.dot(
                pick[...], hidden[:, at], preferred_element_type=F32
            ).astype(BF16)
            return carry

        lax.fori_loop(0, width // tile, select, 0)

        def expert(j, carry):
            rows_j = pl.ds(pl.multiple_of(j * slots, slots), slots)
            both = jnp.dot(arrived[rows_j, :], wbuf[j], preferred_element_type=F32)
            gate = both[:, :ff]
            act[zz, j] = (gate * jax.nn.sigmoid(gate) * both[:, ff:]).astype(BF16)
            return carry

        lax.fori_loop(0, experts, expert, 0)

    step(1)
    across(z)
    for j in range(experts):
        for which in range(2):
            w_copy(j, which).wait()
    compute(z, True)

    def visit(i, carry):
        pl.when(i + 1 < outer)(lambda: step(i + 1))
        zz = near_column(outer, z, i)
        across(zz)
        compute(zz, False)
        return carry

    def place_pages():
        total = jnp.zeros((pages * PAGE, 2 * kvw), F32)
        for n in range(peers):
            if n:
                from_peer(krecv, kvrecv, ksend, n).wait_recv()
            source = lax.rem(ep + n, peers)
            meta = metas[source]
            key = meta[2 * experts : 2 * experts + 1, :]
            goal = meta[2 * experts + 1 : 2 * experts + 2, :]
            want = (lax.broadcasted_iota(jnp.int32, (piece_rows, tok), 0) + ep * piece_rows).astype(F32)
            spread = jnp.where(want == key, 1.0, 0.0).astype(BF16)
            slot = lax.broadcasted_iota(jnp.int32, (pages * PAGE, tok), 0).astype(F32)
            goals = jnp.where(slot == goal, 1.0, 0.0).astype(BF16)
            where = nt_dot(goals, spread).astype(BF16)
            total = total + jnp.dot(where, kvrecv[source], preferred_element_type=F32)
        kv[...] = total.astype(BF16)

    lax.fori_loop(1, outer, visit, 0)
    place_pages()

    def drain(block, carry):
        zz = lax.div(block, inner)
        same = lax.rem(block, inner) == y
        pl.when(same & (z > 0) & (zz >= z))(lambda: block_sent(block, 0))
        pl.when(same & (z < outer - 1) & (zz <= z))(lambda: block_sent(block, 1))
        for n in range(1, inner):
            pl.when(same)(functools.partial(block_sent, block, 1 + n))
        for n in range(1, halves):
            pl.when(block != ep)(functools.partial(block_sent, block, sib_kind + n - 1))
        return carry

    lax.fori_loop(0, peers, drain, 0)
    for n in range(1, peers):
        meta_copy(n).wait_send()
        kv_copy(n).wait_send()


def run_experts(outer, inner, halves, resid, gain, routes, gates, length, keys, values, kgain, cosine, sine, owner, page_slot, wg, wu):
    peers = outer * inner
    tok, width = resid.shape
    cols = width // halves
    experts, _, ff = wg.shape
    slots = -(-inner * CAP // 16) * 16
    meta_rows = -(-(2 * experts + 2) // 8) * 8
    chunks = 4 if peers <= 8 else 2
    kinds = 1 + inner + halves - 1
    kvw = keys.shape[1]
    pages = owner.shape[1]
    dma = pltpu.SemaphoreType.DMA
    vmem = pl.BlockSpec(memory_space=pltpu.VMEM)
    hbm = pl.BlockSpec(memory_space=pl.ANY)
    return pl.pallas_call(
        functools.partial(experts_kernel, outer, inner, halves, chunks),
        out_shape=(
            jax.ShapeDtypeStruct((outer, experts, slots, ff), BF16),
            jax.ShapeDtypeStruct((peers, meta_rows, tok), F32),
            jax.ShapeDtypeStruct((pages * PAGE, 2 * kvw), BF16),
        ),
        in_specs=[hbm] + [vmem] * 11 + [hbm, hbm],
        out_specs=(vmem, vmem, vmem),
        scratch_shapes=[
            pltpu.VMEM((peers, halves, tok, cols), BF16),
            pltpu.VMEM((inner * tok, width), BF16),
            pltpu.VMEM((experts * slots, width), BF16),
            pltpu.VMEM((experts, width, 2 * ff), BF16),
            pltpu.VMEM((experts * slots, inner * tok), BF16),
            pltpu.VMEM((peers, meta_rows, tok), F32),
            pltpu.VMEM((peers, PER_OWNER * PAGE, 2 * kvw), BF16),
            pltpu.VMEM((peers, PER_OWNER * PAGE, 2 * kvw), BF16),
            dma((kinds, peers)),
            dma((peers, halves, chunks)),
            dma((peers,)),
            dma((peers,)),
            dma((peers,)),
            dma((peers,)),
            dma((halves,)),
            dma((2, experts)),
        ],
        compiler_params=pltpu.CompilerParams(
            collective_id=0, has_side_effects=True, vmem_limit_bytes=LIMIT
        ),
        name="run_experts",
    )(resid, gain, routes, gates, length, keys, values, kgain, cosine, sine, owner, page_slot, wg, wu)


def scatter_kernel(
    outer, inner, halves, chunks,
    act, metas, wd, out,
    wbuf, part, pick, sbuf, acc, sib, yb, zb,
    wsem, ssend, srecv, ysend, yrecv, zsend, zrecv,
):
    ep, core, z, y = place(outer, inner)
    other = halves - 1 - core
    tok, cols = out.shape
    experts, ff, width = wd.shape
    slots = act.shape[2]
    piece = tok // chunks
    tile = 512 if cols % 512 == 0 else 128

    def w_copy(j):
        return pltpu.make_async_copy(wd.at[j], wbuf.at[j], wsem.at[j])

    for j in range(experts):
        w_copy(j).start()
    barrier = pltpu.get_barrier_semaphore()

    def signal(to_ep, to_core):
        pl.semaphore_signal(
            barrier, inc=1, device_id={"ep": to_ep, "section": to_core}, device_id_type=MESH
        )

    pl.when(z > 0)(lambda: signal(ep - inner, core))
    pl.when(z < outer - 1)(lambda: signal(ep + inner, core))
    for k in range(1, inner):
        signal(z * inner + lax.rem(y + k, inner), core)
    signal(ep, other)

    def sib_copy(block, slot=0):
        return pltpu.make_async_remote_copy(
            src_ref=sbuf.at[slot],
            dst_ref=sib.at[block],
            send_sem=ssend.at[block],
            recv_sem=srecv.at[block],
            device_id={"ep": ep, "section": other},
            device_id_type=MESH,
        )

    def y_copy(zz, n, k):
        to_y = lax.rem(y + n, inner)
        at = pl.ds(k * piece, piece)
        return pltpu.make_async_remote_copy(
            src_ref=acc.at[zz * inner + to_y, at],
            dst_ref=yb.at[n - 1, zz, at],
            send_sem=ysend.at[n - 1, zz, k],
            recv_sem=yrecv.at[n - 1, zz, k],
            device_id={"ep": z * inner + to_y, "section": core},
            device_id_type=MESH,
        )

    def z_copy(zz, slot, to_ep, k):
        at = pl.ds(k * piece, piece)
        return pltpu.make_async_remote_copy(
            src_ref=acc.at[zz * inner + y, at],
            dst_ref=zb.at[slot, at],
            send_sem=zsend.at[zz, k],
            recv_sem=zrecv.at[slot, k],
            device_id={"ep": to_ep, "section": core},
            device_id_type=MESH,
        )

    def add(dst, k, *sources):
        def body(i, carry):
            at = pl.ds(pl.multiple_of(k * piece + i * 16, 16), 16)
            for c in range(0, cols, tile):
                span = slice(c, c + tile)
                total = sources[0][at, span].astype(F32)
                for source in sources[1:]:
                    total = total + source[at, span].astype(F32)
                dst[at, span] = total.astype(dst.dtype)
            return carry

        lax.fori_loop(0, piece // 16, body, 0)

    def down(zz):
        def expert(j, carry):
            rows_j = pl.ds(pl.multiple_of(j * slots, slots), slots)

            def span(i, carry):
                at = pl.ds(pl.multiple_of(i * tile, tile), tile)
                part[rows_j, at] = jnp.dot(
                    act[zz, j], wbuf[j, :, at], preferred_element_type=F32
                ).astype(BF16)
                return carry

            return lax.fori_loop(0, width // tile, span, carry)

        lax.fori_loop(0, experts, expert, 0)

    def mix(zz, slot):
        meta = [metas[zz * inner + p] for p in range(inner)]
        match = slot_match(meta, 0, experts, slots, inner)
        for p in range(inner):
            weights = [
                jnp.where(match[j][p], meta[p][experts + j : experts + j + 1, :], 0.0)
                for j in range(experts)
            ]
            pick[p * tok : (p + 1) * tok, :] = jnp.concatenate(weights, axis=0).T.astype(BF16)

        def span(half, to_sib):
            def body(i, carry):
                at = pl.ds(pl.multiple_of(half * cols + i * tile, tile), tile)
                to = pl.ds(pl.multiple_of(i * tile, tile), tile)
                mixed = jnp.dot(pick[...], part[:, at], preferred_element_type=F32).astype(BF16)
                for p in range(inner):
                    piece_p = mixed[p * tok : (p + 1) * tok]
                    if to_sib:
                        sbuf[slot + p, :, to] = piece_p
                    else:
                        acc[zz * inner + p, :, to] = piece_p
                return carry

            lax.fori_loop(0, cols // tile, body, 0)

        span(other, True)
        for p in range(inner):
            sib_copy(zz * inner + p, slot + p).start()
        span(core, False)

    def hand_across(zz):
        for n in range(1, inner):
            block = zz * inner + lax.rem(y + n, inner)
            sib_copy(block).wait_recv()
            for k in range(chunks):
                add(acc.at[block], k, acc.at[block], sib.at[block])
                y_copy(zz, n, k).start()

    for j in range(experts):
        w_copy(j).wait()

    def far(i):
        return near_column(outer, z, outer - 1 - i)

    def visit(i, carry):
        zz = far(i)
        slot = lax.rem(i, 2) * inner
        down(zz)

        @pl.when(i == 0)
        def _():
            ends = jnp.where(z > 0, 1, 0) + jnp.where(z < outer - 1, 1, 0)
            pl.semaphore_wait(barrier, ends + inner - 1 + 1)

        @pl.when(i >= 2)
        def _():
            for p in range(inner):
                sib_copy(far(i - 2) * inner + p, slot + p).wait_send()

        mix(zz, slot)
        hand_across(zz)
        return carry

    lax.fori_loop(0, outer, visit, 0)

    def z_step(d, side, zz):
        block = zz * inner + y
        sib_copy(block).wait_recv()
        for k in range(chunks):
            for n in range(1, inner):
                y_copy(zz, n, k).wait_recv()
            parts = [acc.at[block], sib.at[block]] + [yb.at[n, zz] for n in range(inner - 1)]
            feeds = (z - side >= 0) & (z - side < outer)
            first = (d == 1) & (side == -1)
            slot = jnp.where(first, outer, zz)

            @pl.when(feeds)
            def _():
                z_copy(zz, zz, ep, k).wait_recv()
                add(acc.at[block], k, *parts, zb.at[zz])

            @pl.when(jnp.logical_not(feeds))
            def _():
                add(acc.at[block], k, *parts)

            z_copy(zz, slot, ep + side * inner, k).start()

    def last_step():
        block = ep
        sib_copy(block).wait_recv()
        for k in range(chunks):
            for n in range(1, inner):
                y_copy(z, n, k).wait_recv()
            parts = [acc.at[block], sib.at[block]] + [yb.at[n, z] for n in range(inner - 1)]

            @pl.when(z > 0)
            def _():
                z_copy(z, z, ep, k).wait_recv()

            @pl.when(z < outer - 1)
            def _():
                z_copy(z, outer, ep, k).wait_recv()

            @pl.when((z > 0) & (z < outer - 1))
            def _():
                add(out, k, *parts, zb.at[z], zb.at[outer])

            @pl.when((z == 0) & (z < outer - 1))
            def _():
                add(out, k, *parts, zb.at[outer])

            @pl.when((z > 0) & (z == outer - 1))
            def _():
                add(out, k, *parts, zb.at[z])

    def chain(i, carry):
        d = outer - 1 - i
        sides(outer, z, d, functools.partial(z_step, d))
        return carry

    lax.fori_loop(0, outer - 1, chain, 0)
    last_step()

    def close(i, carry):
        d = outer - 1 - i

        def one(side, zz):
            for k in range(chunks):
                z_copy(zz, zz, ep, k).wait_send()

        sides(outer, z, d, one)
        return carry

    lax.fori_loop(0, outer - 1, close, 0)

    def close_across(zz, carry):
        for n in range(1, inner):
            for k in range(chunks):
                y_copy(zz, n, k).wait_send()
        return carry

    lax.fori_loop(0, outer, close_across, 0)
    for i in range(max(0, outer - 2), outer):
        for p in range(inner):
            sib_copy(far(i) * inner + p, (i % 2) * inner + p).wait_send()


def scatter_sums(outer, inner, halves, act, metas, wd):
    peers = outer * inner
    tok = metas.shape[2]
    experts, ff, width = wd.shape
    slots = act.shape[2]
    shape = (tok, width // halves)
    chunks = 4 if peers <= 8 else 2
    dma = pltpu.SemaphoreType.DMA
    across = max(inner - 1, 1)
    lines = outer if inner > 1 else 1
    vmem = pl.BlockSpec(memory_space=pltpu.VMEM)
    return pl.pallas_call(
        functools.partial(scatter_kernel, outer, inner, halves, chunks),
        out_shape=jax.ShapeDtypeStruct(shape, BF16),
        in_specs=[vmem, vmem, pl.BlockSpec(memory_space=pl.ANY)],
        out_specs=vmem,
        scratch_shapes=[
            pltpu.VMEM((experts, ff, width), BF16),
            pltpu.VMEM((experts * slots, width), BF16),
            pltpu.VMEM((inner * tok, experts * slots), BF16),
            pltpu.VMEM((2 * inner,) + shape, BF16),
            pltpu.VMEM((peers,) + shape, BF16),
            pltpu.VMEM((peers,) + shape, BF16),
            pltpu.VMEM((across, lines) + shape, BF16),
            pltpu.VMEM((outer + 1,) + shape, BF16),
            dma((experts,)),
            dma((peers,)),
            dma((peers,)),
            dma((across, outer, chunks)),
            dma((across, outer, chunks)),
            dma((outer, chunks)),
            dma((outer + 1, chunks)),
        ],
        compiler_params=pltpu.CompilerParams(
            collective_id=1, has_side_effects=True, vmem_limit_bytes=LIMIT
        ),
        name="scatter_sums",
    )(act, metas, wd)


def inner_size(mesh):
    try:
        line = mesh.devices[0, :, 0]
        coords = [tuple(device.coords) for device in line]
        inner = 1
        while inner < len(coords) and sum(a != b for a, b in zip(coords[inner], coords[0])) == 1:
            axis = [i for i in range(3) if coords[1][i] != coords[0][i]][0]
            if coords[inner][axis] == coords[0][axis]:
                break
            inner += 1
        return inner if inner < len(coords) and len(coords) % inner == 0 else 1
    except (AttributeError, IndexError, TypeError):
        return 1


def turns(tok, head):
    half = head // 2
    frequency = np.exp(np.arange(half) * (-2.0 / head) * math.log(1000000.0))
    angles = np.arange(tok)[:, None] * frequency
    cosine, sine = np.cos(angles), np.sin(angles)
    return (
        np.concatenate([cosine, cosine], axis=1).astype(np.float32),
        np.concatenate([-sine, sine], axis=1).astype(np.float32),
    )


def shards(
    inner,
    resid,
    norm_gain,
    gate_logits,
    routes,
    w_gate,
    w_up,
    w_down,
    keys_raw,
    values_raw,
    k_gain,
    lengths,
    page_owner,
    page_slot,
):
    halves = lax.axis_size("section")
    outer = lax.axis_size("ep") // inner
    cosine, sine = turns(resid.shape[0], k_gain.shape[0])
    act, metas, kv = run_experts(
        outer, inner, halves,
        resid, norm_gain[None, :], routes, gate_logits, lengths[None, :],
        keys_raw, values_raw, k_gain[None, :], jnp.asarray(cosine), jnp.asarray(sine),
        page_owner, page_slot, w_gate, w_up,
    )
    kv_cache = kv.reshape(page_owner.shape[1], PAGE, 2, keys_raw.shape[1])
    moe_out = scatter_sums(outer, inner, halves, act, metas, w_down)
    return (moe_out, kv_cache)


def solution(mesh):
    in_specs = (
        P(("groups", "ep"), None),
        P(),
        P(("groups", "ep"), None),
        P(("groups", "ep"), None),
        P("ep", None, "section"),
        P("ep", None, "section"),
        P("ep", "section", None),
        P(("groups", "ep"), "section"),
        P(("groups", "ep"), "section"),
        P(),
        P(("groups", "ep")),
        P(("groups", "ep"), None),
        P(("groups", "ep"), None),
    )
    out_specs = (P(("groups", "ep"), "section"), P(("groups", "ep"), None, None, "section"))
    body = functools.partial(shards, inner_size(mesh))
    return jax.shard_map(body, mesh=mesh, in_specs=in_specs, out_specs=out_specs, check_vma=False)
```

```python
import functools
import math

import jax
import jax.numpy as jnp
import numpy as np
from jax import lax
from jax.experimental import pallas as pl
from jax.experimental.pallas import tpu as pltpu
from jax.sharding import PartitionSpec as P

PAGE = 16
CAP = 40
PER_OWNER = 2
F32 = jnp.float32
BF16 = jnp.bfloat16
MESH = pl.DeviceIdType.MESH
LIMIT = 67000000
CHUNKS = 4
SELECT = 2048
MIX = 2048


def place(outer, inner):
    ep = lax.axis_index("ep")
    return ep, lax.axis_index("section"), lax.div(ep, inner), lax.rem(ep, inner)


def near_column(outer, z, i):
    low = jnp.where(2 * z < outer, z, outer - 1 - z)
    step = (i + 1) // 2
    both = jnp.where(i % 2 == 1, step, -step)
    offset = jnp.where(i <= 2 * low, both, i - low)
    return jnp.where(2 * z < outer, z + offset, z - offset)


def sides(outer, z, d, body):
    for side in (-1, 1):
        zz = z + side * d
        pl.when((zz >= 0) & (zz < outer))(functools.partial(body, side, zz))


def nt_dot(a, b):
    return lax.dot_general(a, b, (((1,), (1,)), ((), ())), preferred_element_type=F32)


def slot_match(meta, first, experts, slots, inner):
    rows = []
    tok = meta[0].shape[1]
    slot = lax.broadcasted_iota(jnp.int32, (slots, tok), 0).astype(F32)
    for j in range(experts):
        parts = []
        for p in range(inner):
            rank = meta[p][first + j : first + j + 1, :]
            goal = jnp.where(rank >= 0.0, rank + float(p * CAP), -1.0)
            parts.append(slot == goal)
        rows.append(parts)
    return rows


def experts_kernel(
    outer, inner, halves, chunks,
    resid, gain, routes, gates, length, keys, values, kgain, cosine, sine, owner, page_slot, wg, wu,
    act, metas, kv,
    rows, hidden, arrived, wbuf, pick, msend_buf, kvsend, kvrecv,
    send, recv, msend, mrecv, ksend, krecv, local, wsem,
):
    ep, core, z, y = place(outer, inner)
    peers = outer * inner
    tok, width = resid.shape
    cols = width // halves
    experts, _, ff = wg.shape
    slots = act.shape[2]
    piece = tok // chunks
    sib_kind = 1 + inner
    meta_rows = metas.shape[1]
    pages = owner.shape[1]
    kvw = keys.shape[1]

    def own_copy(h):
        return pltpu.make_async_copy(
            resid.at[:, pl.ds(h * cols, cols)], rows.at[ep, h], local.at[h]
        )

    def w_copy(j, which):
        return pltpu.make_async_copy(
            (wg, wu)[which].at[j], wbuf.at[j, :, pl.ds(which * ff, ff)], wsem.at[which, j]
        )

    for h in range(halves):
        own_copy(h).start()

    barrier = pltpu.get_barrier_semaphore()
    for k in range(1, peers):
        pl.semaphore_signal(
            barrier, inc=1, device_id={"ep": lax.rem(ep + k, peers), "section": core},
            device_id_type=MESH,
        )
    for k in range(1, halves):
        pl.semaphore_signal(
            barrier, inc=1, device_id={"ep": ep, "section": lax.rem(core + k, halves)},
            device_id_type=MESH,
        )
    for j in range(experts):
        for which in range(2):
            w_copy(j, which).start()
    for h in range(halves):
        own_copy(h).wait()
    pl.semaphore_wait(barrier, peers - 1 + halves - 1)

    def chunk_copy(block, half, k, kind, to_ep, to_core):
        at = (block, half, pl.ds(k * piece, piece), slice(None))
        return pltpu.make_async_remote_copy(
            src_ref=rows.at[at],
            dst_ref=rows.at[at],
            send_sem=send.at[kind, block],
            recv_sem=recv.at[block, half, k],
            device_id={"ep": to_ep, "section": to_core},
            device_id_type=MESH,
        )

    def block_sent(block, kind):
        pltpu.make_async_remote_copy(
            src_ref=rows.at[block, core],
            dst_ref=rows.at[block, core],
            send_sem=send.at[kind, block],
            recv_sem=recv.at[block, core, 0],
            device_id={"ep": ep, "section": lax.rem(core + 1, halves)},
            device_id_type=MESH,
        ).wait_send()

    def landed(block, half, k):
        chunk_copy(block, half, k, 0, ep, lax.rem(core + 1, halves)).wait_recv()

    def to_down(block, k):
        chunk_copy(block, core, k, 0, ep - inner, core).start()

    def to_up(block, k):
        chunk_copy(block, core, k, 1, ep + inner, core).start()

    def to_across(block, k):
        for n in range(1, inner):
            chunk_copy(block, core, k, 1 + n, z * inner + lax.rem(y + n, inner), core).start()

    def to_sibling(block, k):
        for n in range(1, halves):
            chunk_copy(
                block, core, k, sib_kind + n - 1, ep, lax.rem(core + n, halves)
            ).start()

    for k in range(chunks):
        pl.when(z > 0)(functools.partial(to_down, ep, k))
        pl.when(z < outer - 1)(functools.partial(to_up, ep, k))
        to_across(ep, k)

    number = experts * peers
    lane = lax.broadcasted_iota(jnp.int32, (1, tok), 1)
    live = lane.astype(F32) < length[...].astype(F32)
    mixing = gates[...] / jnp.sum(gates[...], axis=-1, keepdims=True)
    mixing = mixing.astype(BF16).astype(F32).T
    chosen = routes[...].astype(F32).T
    expert_id = lax.broadcasted_iota(jnp.int32, (number, tok), 0).astype(F32)
    hits = jnp.zeros((number, tok), F32)
    weight = jnp.zeros((number, tok), F32)
    for k in range(chosen.shape[0]):
        same = (chosen[k : k + 1, :] == expert_id) & live
        hits = hits + jnp.where(same, 1.0, 0.0)
        weight = weight + jnp.where(same, mixing[k : k + 1, :], 0.0)
    row_id = lax.broadcasted_iota(jnp.int32, (tok, tok), 0)
    col_id = lax.broadcasted_iota(jnp.int32, (tok, tok), 1)
    earlier = jnp.where(row_id < col_id, 1.0, 0.0).astype(BF16)
    rank = jnp.dot(hits.astype(BF16), earlier, preferred_element_type=F32)
    rank = jnp.where(hits > 0.0, rank, -1.0)

    own_t = jnp.zeros((1, tok), F32)
    slot_t = jnp.zeros((1, tok), F32)
    page_t = lax.div(lane, PAGE)
    for j in range(pages):
        own_t = jnp.where(page_t == j, owner[:, j : j + 1].astype(F32), own_t)
        slot_t = jnp.where(page_t == j, page_slot[:, j : j + 1].astype(F32), slot_t)
    own_here = jnp.broadcast_to(own_t, (tok, tok))
    before = (own_here.T == own_here) & (lax.div(row_id, PAGE) < lax.div(col_id, PAGE))
    order = jnp.sum(jnp.where(before, 1.0, 0.0), axis=0, keepdims=True) * (1.0 / PAGE)
    in_page = (lane - page_t * PAGE).astype(F32)
    key_t = (own_t * PER_OWNER + order) * PAGE + in_page
    goal_t = slot_t * PAGE + in_page
    pad_rows = jnp.zeros((meta_rows - 2 * experts - 2, tok), F32)
    for d in range(peers):
        mine = slice(d * experts, (d + 1) * experts)
        msend_buf[d] = jnp.concatenate([rank[mine], weight[mine], key_t, goal_t, pad_rows], axis=0)

    def meta_copy(n):
        to = lax.rem(ep + n, peers)
        return pltpu.make_async_remote_copy(
            src_ref=msend_buf.at[to],
            dst_ref=metas.at[ep],
            send_sem=msend.at[to],
            recv_sem=mrecv.at[ep],
            device_id={"ep": to, "section": core},
            device_id_type=MESH,
        )

    def kv_copy(n):
        to = lax.rem(ep + n, peers)
        return pltpu.make_async_remote_copy(
            src_ref=kvsend.at[to],
            dst_ref=kvrecv.at[ep],
            send_sem=ksend.at[to],
            recv_sem=krecv.at[ep],
            device_id={"ep": to, "section": core},
            device_id_type=MESH,
        )

    def from_peer(make, buf, sem, n):
        source = lax.rem(ep + n, peers)
        return pltpu.make_async_remote_copy(
            src_ref=buf.at[source],
            dst_ref=buf.at[source],
            send_sem=sem.at[source],
            recv_sem=make.at[source],
            device_id={"ep": source, "section": core},
            device_id_type=MESH,
        )

    for n in range(1, peers):
        meta_copy(n).start()
    metas[ep] = msend_buf[ep]

    live_c = lax.broadcasted_iota(jnp.int32, (tok, 1), 0).astype(F32) < length[...].astype(F32)
    head = kgain.shape[1]
    turned = []
    for h in range(kvw // head):
        x = keys[:, h * head : (h + 1) * head].astype(F32)
        x = x * lax.rsqrt(jnp.mean(x * x, axis=-1, keepdims=True) + 1e-06) * kgain[...].astype(F32)
        swapped = pltpu.roll(x, head // 2, 1)
        x = x * cosine[...] + swapped * sine[...]
        turned.append(jnp.where(live_c, x, 0.0).astype(BF16))
    turned.append(jnp.where(live_c, values[...].astype(F32), 0.0).astype(BF16))
    pairs = jnp.concatenate(turned, axis=1)
    piece_rows = PER_OWNER * PAGE
    group = 1
    while group * piece_rows < 256 and peers % (2 * group) == 0:
        group *= 2
    for d in range(0, peers, group):
        n = group * piece_rows
        want = (lax.broadcasted_iota(jnp.int32, (n, tok), 0) + d * piece_rows).astype(F32)
        chosen_rows = jnp.where(want == key_t, 1.0, 0.0).astype(BF16)
        out = jnp.dot(chosen_rows, pairs, preferred_element_type=F32).astype(BF16)
        for g in range(group):
            kvsend[d + g] = out[g * piece_rows : (g + 1) * piece_rows]
    for n in range(1, peers):
        kv_copy(n).start()
    kvrecv[ep] = kvsend[ep]

    def step(d):
        def body(k, carry):
            def one(side, zz):
                block = zz * inner + y
                landed(block, core, k)
                if side == 1:
                    pl.when(z > 0)(lambda: to_down(block, k))
                else:
                    pl.when(z < outer - 1)(lambda: to_up(block, k))
                to_across(block, k)
                to_sibling(block, k)

            sides(outer, z, d, one)
            return carry

        lax.fori_loop(0, chunks, body, 0)

    def across(zz):
        def body(k, carry):
            for n in range(1, inner):
                block = zz * inner + lax.rem(y + n, inner)
                landed(block, core, k)
                to_sibling(block, k)
            return carry

        lax.fori_loop(0, chunks, body, 0)

    tile = 512 if width % 512 == 0 else 128
    sub = 16

    def normalize(p, block):
        def body(i, carry):
            at = pl.ds(pl.multiple_of(i * sub, sub), sub)
            total = jnp.zeros((sub, 1), F32)
            for h in range(halves):
                for c in range(0, cols, tile):
                    x = rows[block, h, at, c : c + tile].astype(F32)
                    total = total + jnp.sum(x * x, axis=-1, keepdims=True)
            scale = lax.rsqrt(total * (1.0 / width) + 1e-06)
            to = pl.ds(pl.multiple_of(p * tok + i * sub, sub), sub)
            for h in range(halves):
                for c in range(0, cols, tile):
                    x = rows[block, h, at, c : c + tile].astype(F32)
                    g = gain[:, h * cols + c : h * cols + c + tile].astype(F32)
                    hidden[to, h * cols + c : h * cols + c + tile] = (x * scale * g).astype(BF16)
            return carry

        lax.fori_loop(0, tok // sub, body, 0)

    def compute(zz, own):
        for p in range(inner):
            block = zz * inner + p

            def wait_rest(block=block):
                for h in range(1, halves):
                    for k in range(chunks):
                        landed(block, lax.rem(core + h, halves), k)
                from_peer(mrecv, metas, msend, block - ep + peers).wait_recv()

            if own:
                pl.when(block != ep)(wait_rest)
            else:
                wait_rest()
            normalize(p, block)
        meta = [metas[zz * inner + p] for p in range(inner)]
        match = slot_match(meta, 0, experts, slots, inner)
        for j in range(experts):
            for p in range(inner):
                pick[j * slots : (j + 1) * slots, p * tok : (p + 1) * tok] = jnp.where(
                    match[j][p], 1.0, 0.0
                ).astype(BF16)

        def select(i, carry):
            at = pl.ds(pl.multiple_of(i * tile, tile), tile)
            arrived[:, at] = jnp.dot(
                pick[...], hidden[:, at], preferred_element_type=F32
            ).astype(BF16)
            return carry

        lax.fori_loop(0, width // tile, select, 0)

        def expert(j, carry):
            rows_j = pl.ds(pl.multiple_of(j * slots, slots), slots)
            both = jnp.dot(arrived[rows_j, :], wbuf[j], preferred_element_type=F32)
            gate = both[:, :ff]
            act[zz, j] = (gate * jax.nn.sigmoid(gate) * both[:, ff:]).astype(BF16)
            return carry

        lax.fori_loop(0, experts, expert, 0)

    step(1)
    across(z)
    for j in range(experts):
        for which in range(2):
            w_copy(j, which).wait()
    compute(z, True)

    def visit(i, carry):
        pl.when(i + 1 < outer)(lambda: step(i + 1))
        zz = near_column(outer, z, i)
        across(zz)
        compute(zz, False)
        return carry

    def place_pages():
        total = jnp.zeros((pages * PAGE, 2 * kvw), F32)
        for n in range(peers):
            if n:
                from_peer(krecv, kvrecv, ksend, n).wait_recv()
            source = lax.rem(ep + n, peers)
            meta = metas[source]
            key = meta[2 * experts : 2 * experts + 1, :]
            goal = meta[2 * experts + 1 : 2 * experts + 2, :]
            want = (lax.broadcasted_iota(jnp.int32, (piece_rows, tok), 0) + ep * piece_rows).astype(F32)
            spread = jnp.where(want == key, 1.0, 0.0).astype(BF16)
            slot = lax.broadcasted_iota(jnp.int32, (pages * PAGE, tok), 0).astype(F32)
            goals = jnp.where(slot == goal, 1.0, 0.0).astype(BF16)
            where = nt_dot(goals, spread).astype(BF16)
            total = total + jnp.dot(where, kvrecv[source], preferred_element_type=F32)
        kv[...] = total.astype(BF16)

    lax.fori_loop(1, outer, visit, 0)
    place_pages()

    def drain(block, carry):
        zz = lax.div(block, inner)
        same = lax.rem(block, inner) == y
        pl.when(same & (z > 0) & (zz >= z))(lambda: block_sent(block, 0))
        pl.when(same & (z < outer - 1) & (zz <= z))(lambda: block_sent(block, 1))
        for n in range(1, inner):
            pl.when(same)(functools.partial(block_sent, block, 1 + n))
        for n in range(1, halves):
            pl.when(block != ep)(functools.partial(block_sent, block, sib_kind + n - 1))
        return carry

    lax.fori_loop(0, peers, drain, 0)
    for n in range(1, peers):
        meta_copy(n).wait_send()
        kv_copy(n).wait_send()


def run_experts(outer, inner, halves, resid, gain, routes, gates, length, keys, values, kgain, cosine, sine, owner, page_slot, wg, wu):
    peers = outer * inner
    tok, width = resid.shape
    cols = width // halves
    experts, _, ff = wg.shape
    slots = -(-inner * CAP // 16) * 16
    meta_rows = -(-(2 * experts + 2) // 8) * 8
    chunks = 4 if peers <= 8 else 2
    kinds = 1 + inner + halves - 1
    kvw = keys.shape[1]
    pages = owner.shape[1]
    dma = pltpu.SemaphoreType.DMA
    vmem = pl.BlockSpec(memory_space=pltpu.VMEM)
    hbm = pl.BlockSpec(memory_space=pl.ANY)
    return pl.pallas_call(
        functools.partial(experts_kernel, outer, inner, halves, chunks),
        out_shape=(
            jax.ShapeDtypeStruct((outer, experts, slots, ff), BF16),
            jax.ShapeDtypeStruct((peers, meta_rows, tok), F32),
            jax.ShapeDtypeStruct((pages * PAGE, 2 * kvw), BF16),
        ),
        in_specs=[hbm] + [vmem] * 11 + [hbm, hbm],
        out_specs=(vmem, vmem, vmem),
        scratch_shapes=[
            pltpu.VMEM((peers, halves, tok, cols), BF16),
            pltpu.VMEM((inner * tok, width), BF16),
            pltpu.VMEM((experts * slots, width), BF16),
            pltpu.VMEM((experts, width, 2 * ff), BF16),
            pltpu.VMEM((experts * slots, inner * tok), BF16),
            pltpu.VMEM((peers, meta_rows, tok), F32),
            pltpu.VMEM((peers, PER_OWNER * PAGE, 2 * kvw), BF16),
            pltpu.VMEM((peers, PER_OWNER * PAGE, 2 * kvw), BF16),
            dma((kinds, peers)),
            dma((peers, halves, chunks)),
            dma((peers,)),
            dma((peers,)),
            dma((peers,)),
            dma((peers,)),
            dma((halves,)),
            dma((2, experts)),
        ],
        compiler_params=pltpu.CompilerParams(
            collective_id=0, has_side_effects=True, vmem_limit_bytes=LIMIT
        ),
        name="run_experts",
    )(resid, gain, routes, gates, length, keys, values, kgain, cosine, sine, owner, page_slot, wg, wu)


def scatter_kernel(
    outer, inner, halves, chunks,
    act, metas, wd, out,
    wbuf, part, pick, sbuf, acc, sib, yb, zb,
    wsem, ssend, srecv, ysend, yrecv, zsend, zrecv,
):
    ep, core, z, y = place(outer, inner)
    other = halves - 1 - core
    tok, cols = out.shape
    experts, ff, width = wd.shape
    slots = act.shape[2]
    piece = tok // chunks
    tile = 512 if cols % 512 == 0 else 128

    def w_copy(j):
        return pltpu.make_async_copy(wd.at[j], wbuf.at[j], wsem.at[j])

    for j in range(experts):
        w_copy(j).start()
    barrier = pltpu.get_barrier_semaphore()

    def signal(to_ep, to_core):
        pl.semaphore_signal(
            barrier, inc=1, device_id={"ep": to_ep, "section": to_core}, device_id_type=MESH
        )

    pl.when(z > 0)(lambda: signal(ep - inner, core))
    pl.when(z < outer - 1)(lambda: signal(ep + inner, core))
    for k in range(1, inner):
        signal(z * inner + lax.rem(y + k, inner), core)
    signal(ep, other)

    def sib_copy(block, slot=0):
        return pltpu.make_async_remote_copy(
            src_ref=sbuf.at[slot],
            dst_ref=sib.at[block],
            send_sem=ssend.at[block],
            recv_sem=srecv.at[block],
            device_id={"ep": ep, "section": other},
            device_id_type=MESH,
        )

    def y_copy(zz, n, k):
        to_y = lax.rem(y + n, inner)
        at = pl.ds(k * piece, piece)
        return pltpu.make_async_remote_copy(
            src_ref=acc.at[zz * inner + to_y, at],
            dst_ref=yb.at[n - 1, zz, at],
            send_sem=ysend.at[n - 1, zz, k],
            recv_sem=yrecv.at[n - 1, zz, k],
            device_id={"ep": z * inner + to_y, "section": core},
            device_id_type=MESH,
        )

    def z_copy(zz, slot, to_ep, k):
        at = pl.ds(k * piece, piece)
        return pltpu.make_async_remote_copy(
            src_ref=acc.at[zz * inner + y, at],
            dst_ref=zb.at[slot, at],
            send_sem=zsend.at[zz, k],
            recv_sem=zrecv.at[slot, k],
            device_id={"ep": to_ep, "section": core},
            device_id_type=MESH,
        )

    def add(dst, k, *sources):
        def body(i, carry):
            at = pl.ds(pl.multiple_of(k * piece + i * 16, 16), 16)
            for c in range(0, cols, tile):
                span = slice(c, c + tile)
                total = sources[0][at, span].astype(F32)
                for source in sources[1:]:
                    total = total + source[at, span].astype(F32)
                dst[at, span] = total.astype(dst.dtype)
            return carry

        lax.fori_loop(0, piece // 16, body, 0)

    def down(zz):
        def expert(j, carry):
            rows_j = pl.ds(pl.multiple_of(j * slots, slots), slots)

            def span(i, carry):
                at = pl.ds(pl.multiple_of(i * tile, tile), tile)
                part[rows_j, at] = jnp.dot(
                    act[zz, j], wbuf[j, :, at], preferred_element_type=F32
                ).astype(BF16)
                return carry

            return lax.fori_loop(0, width // tile, span, carry)

        lax.fori_loop(0, experts, expert, 0)

    def mix(zz, slot):
        meta = [metas[zz * inner + p] for p in range(inner)]
        match = slot_match(meta, 0, experts, slots, inner)
        for p in range(inner):
            weights = [
                jnp.where(match[j][p], meta[p][experts + j : experts + j + 1, :], 0.0)
                for j in range(experts)
            ]
            pick[p * tok : (p + 1) * tok, :] = jnp.concatenate(weights, axis=0).T.astype(BF16)

        def span(half, to_sib):
            def body(i, carry):
                at = pl.ds(pl.multiple_of(half * cols + i * tile, tile), tile)
                to = pl.ds(pl.multiple_of(i * tile, tile), tile)
                mixed = jnp.dot(pick[...], part[:, at], preferred_element_type=F32).astype(BF16)
                for p in range(inner):
                    piece_p = mixed[p * tok : (p + 1) * tok]
                    if to_sib:
                        sbuf[slot + p, :, to] = piece_p
                    else:
                        acc[zz * inner + p, :, to] = piece_p
                return carry

            lax.fori_loop(0, cols // tile, body, 0)

        span(other, True)
        for p in range(inner):
            sib_copy(zz * inner + p, slot + p).start()
        span(core, False)

    def hand_across(zz):
        for n in range(1, inner):
            block = zz * inner + lax.rem(y + n, inner)
            sib_copy(block).wait_recv()
            for k in range(chunks):
                add(acc.at[block], k, acc.at[block], sib.at[block])
                y_copy(zz, n, k).start()

    for j in range(experts):
        w_copy(j).wait()

    def far(i):
        return near_column(outer, z, outer - 1 - i)

    def visit(i, carry):
        zz = far(i)
        slot = lax.rem(i, 2) * inner
        down(zz)

        @pl.when(i == 0)
        def _():
            ends = jnp.where(z > 0, 1, 0) + jnp.where(z < outer - 1, 1, 0)
            pl.semaphore_wait(barrier, ends + inner - 1 + 1)

        @pl.when(i >= 2)
        def _():
            for p in range(inner):
                sib_copy(far(i - 2) * inner + p, slot + p).wait_send()

        mix(zz, slot)
        hand_across(zz)
        return carry

    lax.fori_loop(0, outer, visit, 0)

    def z_step(d, side, zz):
        block = zz * inner + y
        sib_copy(block).wait_recv()
        for k in range(chunks):
            for n in range(1, inner):
                y_copy(zz, n, k).wait_recv()
            parts = [acc.at[block], sib.at[block]] + [yb.at[n, zz] for n in range(inner - 1)]
            feeds = (z - side >= 0) & (z - side < outer)
            first = (d == 1) & (side == -1)
            slot = jnp.where(first, outer, zz)

            @pl.when(feeds)
            def _():
                z_copy(zz, zz, ep, k).wait_recv()
                add(acc.at[block], k, *parts, zb.at[zz])

            @pl.when(jnp.logical_not(feeds))
            def _():
                add(acc.at[block], k, *parts)

            z_copy(zz, slot, ep + side * inner, k).start()

    def last_step():
        block = ep
        sib_copy(block).wait_recv()
        for k in range(chunks):
            for n in range(1, inner):
                y_copy(z, n, k).wait_recv()
            parts = [acc.at[block], sib.at[block]] + [yb.at[n, z] for n in range(inner - 1)]

            @pl.when(z > 0)
            def _():
                z_copy(z, z, ep, k).wait_recv()

            @pl.when(z < outer - 1)
            def _():
                z_copy(z, outer, ep, k).wait_recv()

            @pl.when((z > 0) & (z < outer - 1))
            def _():
                add(out, k, *parts, zb.at[z], zb.at[outer])

            @pl.when((z == 0) & (z < outer - 1))
            def _():
                add(out, k, *parts, zb.at[outer])

            @pl.when((z > 0) & (z == outer - 1))
            def _():
                add(out, k, *parts, zb.at[z])

    def chain(i, carry):
        d = outer - 1 - i
        sides(outer, z, d, functools.partial(z_step, d))
        return carry

    lax.fori_loop(0, outer - 1, chain, 0)
    last_step()

    def close(i, carry):
        d = outer - 1 - i

        def one(side, zz):
            for k in range(chunks):
                z_copy(zz, zz, ep, k).wait_send()

        sides(outer, z, d, one)
        return carry

    lax.fori_loop(0, outer - 1, close, 0)

    def close_across(zz, carry):
        for n in range(1, inner):
            for k in range(chunks):
                y_copy(zz, n, k).wait_send()
        return carry

    lax.fori_loop(0, outer, close_across, 0)
    for i in range(max(0, outer - 2), outer):
        for p in range(inner):
            sib_copy(far(i) * inner + p, (i % 2) * inner + p).wait_send()


def scatter_sums(outer, inner, halves, act, metas, wd):
    peers = outer * inner
    tok = metas.shape[2]
    experts, ff, width = wd.shape
    slots = act.shape[2]
    shape = (tok, width // halves)
    chunks = 4 if peers <= 8 else 2
    dma = pltpu.SemaphoreType.DMA
    across = max(inner - 1, 1)
    lines = outer if inner > 1 else 1
    vmem = pl.BlockSpec(memory_space=pltpu.VMEM)
    return pl.pallas_call(
        functools.partial(scatter_kernel, outer, inner, halves, chunks),
        out_shape=jax.ShapeDtypeStruct(shape, BF16),
        in_specs=[vmem, vmem, pl.BlockSpec(memory_space=pl.ANY)],
        out_specs=vmem,
        scratch_shapes=[
            pltpu.VMEM((experts, ff, width), BF16),
            pltpu.VMEM((experts * slots, width), BF16),
            pltpu.VMEM((inner * tok, experts * slots), BF16),
            pltpu.VMEM((2 * inner,) + shape, BF16),
            pltpu.VMEM((peers,) + shape, BF16),
            pltpu.VMEM((peers,) + shape, BF16),
            pltpu.VMEM((across, lines) + shape, BF16),
            pltpu.VMEM((outer + 1,) + shape, BF16),
            dma((experts,)),
            dma((peers,)),
            dma((peers,)),
            dma((across, outer, chunks)),
            dma((across, outer, chunks)),
            dma((outer, chunks)),
            dma((outer + 1, chunks)),
        ],
        compiler_params=pltpu.CompilerParams(
            collective_id=1, has_side_effects=True, vmem_limit_bytes=LIMIT
        ),
        name="scatter_sums",
    )(act, metas, wd)


def layer_kernel(
    outer, inner, halves, chunks,
    resid, gain, routes, gates, length, keys, values, kgain, cosine, sine, owner, page_slot, wg, wu, wd,
    out, kv,
    rows, sib, yb, zb, arrived, wbuf, dbuf, act, pick, comb, scale, metas, msend_buf, kvsend, kvrecv,
    send, recv, msend, mrecv, ksend, krecv, local, wsem, dsem, ssend, srecv, ysend, yrecv, zsend, zrecv,
):
    ep, core, z, y = place(outer, inner)
    other = halves - 1 - core
    peers = outer * inner
    tok, width = resid.shape
    cols = width // halves
    experts, _, ff = wg.shape
    slots = act.shape[2]
    piece = tok // chunks
    sib_kind = 1 + inner
    meta_rows = metas.shape[1]
    pages = owner.shape[1]
    kvw = keys.shape[1]
    tile = 512 if cols % 512 == 0 else 128

    def remote(src, dst, send_sem, recv_sem, to_ep, to_core):
        return pltpu.make_async_remote_copy(
            src_ref=src, dst_ref=dst, send_sem=send_sem, recv_sem=recv_sem,
            device_id={"ep": to_ep, "section": to_core}, device_id_type=MESH,
        )

    def own_copy(h):
        return pltpu.make_async_copy(
            resid.at[:, pl.ds(h * cols, cols)], rows.at[ep, h], local.at[h]
        )

    def w_copy(j, which):
        return pltpu.make_async_copy(
            (wg, wu)[which].at[j], wbuf.at[j, :, pl.ds(which * ff, ff)], wsem.at[which, j]
        )

    def d_copy(j):
        return pltpu.make_async_copy(wd.at[j], dbuf.at[j], dsem.at[j])

    for h in range(halves):
        own_copy(h).start()
    barrier = pltpu.get_barrier_semaphore()

    def greet(to_ep, to_core):
        pl.semaphore_signal(
            barrier, inc=1, device_id={"ep": to_ep, "section": to_core}, device_id_type=MESH
        )

    for k in range(1, peers):
        greet(lax.rem(ep + k, peers), core)
    greet(ep, other)
    for j in range(experts):
        for which in range(2):
            w_copy(j, which).start()
    for j in range(experts):
        d_copy(j).start()
    for h in range(halves):
        own_copy(h).wait()
    pl.semaphore_wait(barrier, peers - 1 + 1)

    def chunk_copy(block, half, k, kind, to_ep, to_core):
        at = (block, half, pl.ds(k * piece, piece), slice(None))
        return remote(
            rows.at[at], rows.at[at], send.at[kind, block], recv.at[block, half, k], to_ep, to_core
        )

    def block_sent(block, kind):
        whole = rows.at[block, core]
        remote(whole, whole, send.at[kind, block], recv.at[block, core, 0], ep, other).wait_send()

    def landed(block, half, k):
        chunk_copy(block, half, k, 0, ep, other).wait_recv()

    def to_down(block, k):
        chunk_copy(block, core, k, 0, ep - inner, core).start()

    def to_up(block, k):
        chunk_copy(block, core, k, 1, ep + inner, core).start()

    def to_across(block, k):
        for n in range(1, inner):
            chunk_copy(block, core, k, 1 + n, z * inner + lax.rem(y + n, inner), core).start()

    def to_sibling(block, k):
        chunk_copy(block, core, k, sib_kind, ep, other).start()

    for k in range(chunks):
        pl.when(z > 0)(functools.partial(to_down, ep, k))
        pl.when(z < outer - 1)(functools.partial(to_up, ep, k))
        to_across(ep, k)

    number = experts * peers
    lane = lax.broadcasted_iota(jnp.int32, (1, tok), 1)
    live = lane.astype(F32) < length[...].astype(F32)
    mixing = gates[...] / jnp.sum(gates[...], axis=0, keepdims=True)
    mixing = mixing.astype(BF16).astype(F32)
    chosen = routes[...].astype(F32)
    expert_id = lax.broadcasted_iota(jnp.int32, (number, tok), 0).astype(F32)
    hits = jnp.zeros((number, tok), F32)
    weight = jnp.zeros((number, tok), F32)
    for k in range(chosen.shape[0]):
        same = (chosen[k : k + 1, :] == expert_id) & live
        hits = hits + jnp.where(same, 1.0, 0.0)
        weight = weight + jnp.where(same, mixing[k : k + 1, :], 0.0)
    row_id = lax.broadcasted_iota(jnp.int32, (tok, tok), 0)
    col_id = lax.broadcasted_iota(jnp.int32, (tok, tok), 1)
    earlier = jnp.where(row_id < col_id, 1.0, 0.0).astype(BF16)
    rank = jnp.dot(hits.astype(BF16), earlier, preferred_element_type=F32)
    rank = jnp.where(hits > 0.0, rank, -1.0)

    own_t = jnp.zeros((1, tok), F32)
    slot_t = jnp.zeros((1, tok), F32)
    page_t = lax.div(lane, PAGE)
    for j in range(pages):
        own_t = jnp.where(page_t == j, owner[:, j : j + 1].astype(F32), own_t)
        slot_t = jnp.where(page_t == j, page_slot[:, j : j + 1].astype(F32), slot_t)
    own_here = jnp.broadcast_to(own_t, (tok, tok))
    before = (own_here.T == own_here) & (lax.div(row_id, PAGE) < lax.div(col_id, PAGE))
    order = jnp.sum(jnp.where(before, 1.0, 0.0), axis=0, keepdims=True) * (1.0 / PAGE)
    in_page = (lane - page_t * PAGE).astype(F32)
    key_t = (own_t * PER_OWNER + order) * PAGE + in_page
    goal_t = slot_t * PAGE + in_page
    pad_rows = jnp.zeros((meta_rows - 2 * experts - 2, tok), F32)
    for d in range(peers):
        mine = slice(d * experts, (d + 1) * experts)
        msend_buf[d] = jnp.concatenate([rank[mine], weight[mine], key_t, goal_t, pad_rows], axis=0)

    def meta_copy(n):
        to = lax.rem(ep + n, peers)
        return remote(msend_buf.at[to], metas.at[ep], msend.at[to], mrecv.at[ep], to, core)

    def kv_copy(n):
        to = lax.rem(ep + n, peers)
        return remote(kvsend.at[to], kvrecv.at[ep], ksend.at[to], krecv.at[ep], to, core)

    def meta_landed(block):
        remote(
            metas.at[block], metas.at[block], msend.at[block], mrecv.at[block], block, core
        ).wait_recv()

    def kv_landed(block):
        remote(
            kvrecv.at[block], kvrecv.at[block], ksend.at[block], krecv.at[block], block, core
        ).wait_recv()

    for n in range(1, peers):
        meta_copy(n).start()
    metas[ep] = msend_buf[ep]

    piece_rows = PER_OWNER * PAGE

    def prepare_pages():
        live_c = lax.broadcasted_iota(jnp.int32, (tok, 1), 0).astype(F32) < length[...].astype(F32)
        head = kgain.shape[1]
        turned = []
        for h in range(kvw // head):
            x = keys[:, h * head : (h + 1) * head].astype(F32)
            mean_square = jnp.mean(x * x, axis=-1, keepdims=True)
            x = x * lax.rsqrt(mean_square + 1e-06) * kgain[...].astype(F32)
            swapped = pltpu.roll(x, head // 2, 1)
            x = x * cosine[...] + swapped * sine[...]
            turned.append(jnp.where(live_c, x, 0.0).astype(BF16))
        turned.append(jnp.where(live_c, values[...].astype(F32), 0.0).astype(BF16))
        pairs = jnp.concatenate(turned, axis=1)
        group = 1
        while group * piece_rows < 256 and peers % (2 * group) == 0:
            group *= 2
        for d in range(0, peers, group):
            n = group * piece_rows
            want = (lax.broadcasted_iota(jnp.int32, (n, tok), 0) + d * piece_rows).astype(F32)
            chosen_rows = jnp.where(want == key_t, 1.0, 0.0).astype(BF16)
            picked = jnp.dot(chosen_rows, pairs, preferred_element_type=F32).astype(BF16)
            for g in range(group):
                kvsend[d + g] = picked[g * piece_rows : (g + 1) * piece_rows]
        kvrecv[ep] = kvsend[ep]

    def place_pages():
        total = jnp.zeros((pages * PAGE, 2 * kvw), F32)
        for n in range(peers):
            source = lax.rem(ep + n, peers)
            if n:
                kv_landed(source)
            meta = metas[source]
            key = meta[2 * experts : 2 * experts + 1, :]
            goal = meta[2 * experts + 1 : 2 * experts + 2, :]
            want = (lax.broadcasted_iota(jnp.int32, (piece_rows, tok), 0) + ep * piece_rows).astype(F32)
            spread = jnp.where(want == key, 1.0, 0.0).astype(BF16)
            slot = lax.broadcasted_iota(jnp.int32, (pages * PAGE, tok), 0).astype(F32)
            goals = jnp.where(slot == goal, 1.0, 0.0).astype(BF16)
            where = nt_dot(goals, spread).astype(BF16)
            total = total + jnp.dot(where, kvrecv[source], preferred_element_type=F32)
        kv[...] = total.astype(BF16)

    def step(d):
        def body(k, carry):
            def one(side, zz):
                block = zz * inner + y
                landed(block, core, k)
                if side == 1:
                    pl.when(z > 0)(lambda: to_down(block, k))
                else:
                    pl.when(z < outer - 1)(lambda: to_up(block, k))
                to_across(block, k)
                to_sibling(block, k)

            sides(outer, z, d, one)
            return carry

        lax.fori_loop(0, chunks, body, 0)

    def across(zz):
        def body(k, carry):
            for n in range(1, inner):
                block = zz * inner + lax.rem(y + n, inner)
                landed(block, core, k)
                to_sibling(block, k)
            return carry

        lax.fori_loop(0, chunks, body, 0)

    sub = 16

    def row_scales(block, p, k):
        for i in range(piece // sub):
            at = pl.ds(pl.multiple_of(k * piece + i * sub, sub), sub)
            total = jnp.zeros((sub, tile), F32)
            for h in range(halves):
                for c in range(0, cols, tile):
                    x = rows[block, h, at, c : c + tile].astype(F32)
                    total = total + x * x
            mean_square = jnp.sum(total, axis=-1, keepdims=True) * (1.0 / width)
            to = pl.ds(pl.multiple_of(p * tok + k * piece + i * sub, sub), sub)
            scale[to, :] = jnp.broadcast_to(lax.rsqrt(mean_square + 1e-06), (sub, 128))

    def other_half(block, p, own):
        def body(k, carry):
            if own:
                pl.when(block != ep)(lambda: landed(block, other, k))
            else:
                landed(block, other, k)
            row_scales(block, p, k)
            return carry

        lax.fori_loop(0, chunks, body, 0)

    def hidden_layer(zz, own):
        for n in range(inner):
            p = lax.rem(y + n, inner)
            block = zz * inner + p
            other_half(block, p, own and n == 0)
            if own and n == 0:
                continue
            meta_landed(block)
        meta = [metas[zz * inner + p] for p in range(inner)]
        match = slot_match(meta, 0, experts, slots, inner)
        factors = []
        lanes = [
            scale[p * tok : (p + 1) * tok, :tok].T[0:1, :] for p in range(inner)
        ]
        for j in range(experts):
            factor = jnp.zeros((slots, 1), F32)
            for p in range(inner):
                pick[j * slots : (j + 1) * slots, p * tok : (p + 1) * tok] = jnp.where(
                    match[j][p], 1.0, 0.0
                ).astype(BF16)
                factor = factor + jnp.sum(
                    jnp.where(match[j][p], lanes[p], 0.0), axis=-1, keepdims=True
                )
            factors.append(factor)
        factor = jnp.concatenate(factors, axis=0)
        span = min(cols, SELECT)
        for h in range(halves):
            def select(i, carry, h=h):
                at = pl.ds(pl.multiple_of(i * span, span), span)
                to = pl.ds(pl.multiple_of(h * cols + i * span, span), span)
                source = rows[pl.ds(zz * inner, inner), h, :, at].reshape(inner * tok, span)
                found = jnp.dot(pick[...], source, preferred_element_type=F32)
                arrived[:, to] = (found * factor * gain[:, to].astype(F32)).astype(BF16)
                return carry

            lax.fori_loop(0, cols // span, select, 0)

        def expert(j, carry):
            rows_j = pl.ds(pl.multiple_of(j * slots, slots), slots)
            both = jnp.dot(arrived[rows_j, :], wbuf[j], preferred_element_type=F32)
            gate = both[:, :ff]
            act[zz, j] = (gate * jax.nn.sigmoid(gate) * both[:, ff:]).astype(BF16)
            return carry

        lax.fori_loop(0, experts, expert, 0)

    def sib_copy(block):
        return remote(rows.at[block, other], sib.at[block], ssend.at[block], srecv.at[block], ep, other)

    def y_copy(zz, n, k):
        to_y = lax.rem(y + n, inner)
        at = pl.ds(k * piece, piece)
        return remote(
            rows.at[zz * inner + to_y, core, at], yb.at[n - 1, zz, at],
            ysend.at[n - 1, zz, k], yrecv.at[n - 1, zz, k], z * inner + to_y, core,
        )

    def z_copy(zz, slot, to_ep, k):
        at = pl.ds(k * piece, piece)
        return remote(
            rows.at[zz * inner + y, core, at], zb.at[slot, at],
            zsend.at[zz, k], zrecv.at[slot, k], to_ep, core,
        )

    def add(dst, k, *sources):
        def body(i, carry):
            at = pl.ds(pl.multiple_of(k * piece + i * 16, 16), 16)
            for c in range(0, cols, tile):
                part = slice(c, c + tile)
                total = sources[0][at, part].astype(F32)
                for source in sources[1:]:
                    total = total + source[at, part].astype(F32)
                dst[at, part] = total.astype(dst.dtype)
            return carry

        lax.fori_loop(0, piece // 16, body, 0)

    def output_layer(zz):
        for p in range(inner):
            block = zz * inner + p
            same = y == p
            pl.when(same & (z > 0) & (zz >= z))(functools.partial(block_sent, block, 0))
            pl.when(same & (z < outer - 1) & (zz <= z))(functools.partial(block_sent, block, 1))
            for n in range(1, inner):
                pl.when(same)(functools.partial(block_sent, block, 1 + n))
            pl.when(block != ep)(functools.partial(block_sent, block, sib_kind))
        meta = [metas[zz * inner + p] for p in range(inner)]
        match = slot_match(meta, 0, experts, slots, inner)
        for p in range(inner):
            weights = [
                jnp.where(match[j][p], meta[p][experts + j : experts + j + 1, :], 0.0)
                for j in range(experts)
            ]
            comb[p * tok : (p + 1) * tok, :] = jnp.concatenate(weights, axis=0).T.astype(BF16)

        def half_of(half, to_sib):
            at = pl.ds(pl.multiple_of(half * cols, cols), cols)

            def expert(j, carry):
                rows_j = pl.ds(pl.multiple_of(j * slots, slots), slots)
                arrived[rows_j, at] = jnp.dot(
                    act[zz, j], dbuf[j, :, at], preferred_element_type=F32
                ).astype(BF16)
                return carry

            lax.fori_loop(0, experts, expert, 0)
            span = min(cols, MIX)

            def body(i, carry):
                at = pl.ds(pl.multiple_of(half * cols + i * span, span), span)
                to = pl.ds(pl.multiple_of(i * span, span), span)
                mixed = jnp.dot(comb[...], arrived[:, at], preferred_element_type=F32).astype(BF16)
                for p in range(inner):
                    rows[zz * inner + p, half, :, to] = mixed[p * tok : (p + 1) * tok]
                return carry

            lax.fori_loop(0, cols // span, body, 0)
            if to_sib:
                for p in range(inner):
                    sib_copy(zz * inner + p).start()

        half_of(other, True)
        half_of(core, False)

    def hand_across(zz):
        for n in range(1, inner):
            block = zz * inner + lax.rem(y + n, inner)
            sib_copy(block).wait_recv()
            for k in range(chunks):
                add(rows.at[block, core], k, rows.at[block, core], sib.at[block])
                y_copy(zz, n, k).start()

    def z_step(d, side, zz):
        block = zz * inner + y
        mine = rows.at[block, core]
        sib_copy(block).wait_recv()
        for k in range(chunks):
            for n in range(1, inner):
                y_copy(zz, n, k).wait_recv()
            parts = [mine, sib.at[block]] + [yb.at[n, zz] for n in range(inner - 1)]
            feeds = (z - side >= 0) & (z - side < outer)
            slot = outer if (d == 1 and side == -1) else zz

            @pl.when(feeds)
            def _():
                z_copy(zz, zz, ep, k).wait_recv()
                add(mine, k, *parts, zb.at[zz])

            @pl.when(jnp.logical_not(feeds))
            def _():
                add(mine, k, *parts)

            z_copy(zz, slot, ep + side * inner, k).start()

    def last_step():
        sib_copy(ep).wait_recv()
        for k in range(chunks):
            for n in range(1, inner):
                y_copy(z, n, k).wait_recv()
            parts = [rows.at[ep, core], sib.at[ep]] + [yb.at[n, z] for n in range(inner - 1)]
            pl.when(z > 0)(lambda: z_copy(z, z, ep, k).wait_recv())
            pl.when(z < outer - 1)(lambda: z_copy(z, outer, ep, k).wait_recv())
            pl.when((z > 0) & (z < outer - 1))(
                lambda: add(out, k, *parts, zb.at[z], zb.at[outer])
            )
            pl.when((z == 0) & (z < outer - 1))(lambda: add(out, k, *parts, zb.at[outer]))
            pl.when((z > 0) & (z == outer - 1))(lambda: add(out, k, *parts, zb.at[z]))

    columns = [near_column(outer, z, i) for i in range(outer)]
    prepare_pages()
    for i in range(outer):
        if i + 1 < outer:
            step(i + 1)
        if i == max(outer - 2, 0):
            for n in range(1, peers):
                kv_copy(n).start()
        across(columns[i])
        if i == 0:
            for j in range(experts):
                for which in range(2):
                    w_copy(j, which).wait()
        hidden_layer(columns[i], i == 0)
        if i == 0:
            for j in range(experts):
                d_copy(j).wait()
        if i == 1 and outer > 2:
            output_layer(columns[0])
        if i >= outer - 2:
            output_layer(columns[i])
            hand_across(columns[i])
    for i in range(outer - 3, -1, -1):
        if i > 0 or outer <= 2:
            output_layer(columns[i])
        hand_across(columns[i])
    for d in range(outer - 1, 0, -1):
        sides(outer, z, d, functools.partial(z_step, d))
        if d == outer - 1:
            place_pages()
    last_step()

    for d in range(outer - 1, 0, -1):
        def sent(side, zz):
            for k in range(chunks):
                z_copy(zz, zz, ep, k).wait_send()

        sides(outer, z, d, sent)
    for zz in range(outer):
        for n in range(1, inner):
            for k in range(chunks):
                y_copy(zz, n, k).wait_send()
    for block in range(peers):
        sib_copy(block).wait_send()
    for n in range(1, peers):
        meta_copy(n).wait_send()
        kv_copy(n).wait_send()


def run_layer(outer, inner, halves, resid, gain, routes, gates, length, keys, values, kgain, cosine, sine, owner, page_slot, wg, wu, wd):
    peers = outer * inner
    tok, width = resid.shape
    cols = width // halves
    experts, _, ff = wg.shape
    slots = -(-inner * CAP // 16) * 16
    meta_rows = -(-(2 * experts + 2) // 8) * 8
    chunks = CHUNKS
    kinds = 1 + inner + halves - 1
    kvw = keys.shape[1]
    pages = owner.shape[1]
    across = max(inner - 1, 1)
    lines = outer if inner > 1 else 1
    dma = pltpu.SemaphoreType.DMA
    vmem = pl.BlockSpec(memory_space=pltpu.VMEM)
    hbm = pl.BlockSpec(memory_space=pl.ANY)
    return pl.pallas_call(
        functools.partial(layer_kernel, outer, inner, halves, chunks),
        out_shape=(
            jax.ShapeDtypeStruct((tok, cols), BF16),
            jax.ShapeDtypeStruct((pages * PAGE, 2 * kvw), BF16),
        ),
        in_specs=[hbm] + [vmem] * 11 + [hbm] * 3,
        out_specs=(vmem, vmem),
        scratch_shapes=[
            pltpu.VMEM((peers, halves, tok, cols), BF16),
            pltpu.VMEM((peers, tok, cols), BF16),
            pltpu.VMEM((across, lines, tok, cols), BF16),
            pltpu.VMEM((outer + 1, tok, cols), BF16),
            pltpu.VMEM((experts * slots, width), BF16),
            pltpu.VMEM((experts, width, 2 * ff), BF16),
            pltpu.VMEM((experts, ff, width), BF16),
            pltpu.VMEM((outer, experts, slots, ff), BF16),
            pltpu.VMEM((experts * slots, inner * tok), BF16),
            pltpu.VMEM((inner * tok, experts * slots), BF16),
            pltpu.VMEM((inner * tok, 128), F32),
            pltpu.VMEM((peers, meta_rows, tok), F32),
            pltpu.VMEM((peers, meta_rows, tok), F32),
            pltpu.VMEM((peers, PER_OWNER * PAGE, 2 * kvw), BF16),
            pltpu.VMEM((peers, PER_OWNER * PAGE, 2 * kvw), BF16),
            dma((kinds, peers)),
            dma((peers, halves, chunks)),
            dma((peers,)),
            dma((peers,)),
            dma((peers,)),
            dma((peers,)),
            dma((halves,)),
            dma((2, experts)),
            dma((experts,)),
            dma((peers,)),
            dma((peers,)),
            dma((across, outer, chunks)),
            dma((across, outer, chunks)),
            dma((outer, chunks)),
            dma((outer + 1, chunks)),
        ],
        compiler_params=pltpu.CompilerParams(
            collective_id=0, has_side_effects=True, vmem_limit_bytes=LIMIT
        ),
        name="run_layer",
    )(resid, gain, routes, gates, length, keys, values, kgain, cosine, sine, owner, page_slot, wg, wu, wd)


def fits(outer, inner, halves, tok, width, experts, ff):
    peers = outer * inner
    block = tok * width // halves * 2
    rows = (halves * peers + peers + outer * (inner - 1) + outer + 1) * block
    return rows + 6 * experts * ff * width + 4 * experts * inner * CAP * width < LIMIT


def inner_size(mesh):
    try:
        line = mesh.devices[0, :, 0]
        coords = [tuple(device.coords) for device in line]
        inner = 1
        while inner < len(coords) and sum(a != b for a, b in zip(coords[inner], coords[0])) == 1:
            axis = [i for i in range(3) if coords[1][i] != coords[0][i]][0]
            if coords[inner][axis] == coords[0][axis]:
                break
            inner += 1
        return inner if inner < len(coords) and len(coords) % inner == 0 else 1
    except (AttributeError, IndexError, TypeError):
        return 1


def turns(tok, head):
    half = head // 2
    frequency = np.exp(np.arange(half) * (-2.0 / head) * math.log(1000000.0))
    angles = np.arange(tok)[:, None] * frequency
    cosine, sine = np.cos(angles), np.sin(angles)
    return (
        np.concatenate([cosine, cosine], axis=1).astype(np.float32),
        np.concatenate([-sine, sine], axis=1).astype(np.float32),
    )


def shards(
    inner,
    resid,
    norm_gain,
    gate_logits,
    routes,
    w_gate,
    w_up,
    w_down,
    keys_raw,
    values_raw,
    k_gain,
    lengths,
    page_owner,
    page_slot,
):
    halves = lax.axis_size("section")
    outer = lax.axis_size("ep") // inner
    cosine, sine = turns(resid.shape[0], k_gain.shape[0])
    tok, width = resid.shape
    if fits(outer, inner, halves, tok, width, w_gate.shape[0], w_gate.shape[2]):
        moe_out, kv = run_layer(
            outer, inner, halves,
            resid, norm_gain[None, :], routes.T, gate_logits.T, lengths[None, :],
            keys_raw, values_raw, k_gain[None, :], jnp.asarray(cosine), jnp.asarray(sine),
            page_owner, page_slot, w_gate, w_up, w_down,
        )
        return (moe_out, kv.reshape(page_owner.shape[1], PAGE, 2, keys_raw.shape[1]))
    act, metas, kv = run_experts(
        outer, inner, halves,
        resid, norm_gain[None, :], routes, gate_logits, lengths[None, :],
        keys_raw, values_raw, k_gain[None, :], jnp.asarray(cosine), jnp.asarray(sine),
        page_owner, page_slot, w_gate, w_up,
    )
    kv_cache = kv.reshape(page_owner.shape[1], PAGE, 2, keys_raw.shape[1])
    moe_out = scatter_sums(outer, inner, halves, act, metas, w_down)
    return (moe_out, kv_cache)


def solution(mesh):
    in_specs = (
        P(("groups", "ep"), None),
        P(),
        P(("groups", "ep"), None),
        P(("groups", "ep"), None),
        P("ep", None, "section"),
        P("ep", None, "section"),
        P("ep", "section", None),
        P(("groups", "ep"), "section"),
        P(("groups", "ep"), "section"),
        P(),
        P(("groups", "ep")),
        P(("groups", "ep"), None),
        P(("groups", "ep"), None),
    )
    out_specs = (P(("groups", "ep"), "section"), P(("groups", "ep"), None, None, "section"))
    body = functools.partial(shards, inner_size(mesh))
    return jax.shard_map(body, mesh=mesh, in_specs=in_specs, out_specs=out_specs, check_vma=False)
```

```python
import functools
import math

import jax
import jax.numpy as jnp
import numpy as np
from jax import lax
from jax.experimental import pallas as pl
from jax.experimental.pallas import tpu as pltpu
from jax.sharding import PartitionSpec as P

PAGE = 16
CAP = 40
PER_OWNER = 2
F32 = jnp.float32
BF16 = jnp.bfloat16
MESH = pl.DeviceIdType.MESH
LIMIT = 67000000
CHUNKS = 4
SELECT = 2048
MIX = 2048


def place(outer, inner):
    ep = lax.axis_index("ep")
    return ep, lax.axis_index("section"), lax.div(ep, inner), lax.rem(ep, inner)


def near_column(outer, z, i):
    low = jnp.where(2 * z < outer, z, outer - 1 - z)
    step = (i + 1) // 2
    both = jnp.where(i % 2 == 1, step, -step)
    offset = jnp.where(i <= 2 * low, both, i - low)
    return jnp.where(2 * z < outer, z + offset, z - offset)


def sides(outer, z, d, body):
    for side in (-1, 1):
        zz = z + side * d
        pl.when((zz >= 0) & (zz < outer))(functools.partial(body, side, zz))


def nt_dot(a, b):
    return lax.dot_general(a, b, (((1,), (1,)), ((), ())), preferred_element_type=F32)


def slot_match(meta, first, experts, slots, inner):
    rows = []
    tok = meta[0].shape[1]
    slot = lax.broadcasted_iota(jnp.int32, (slots, tok), 0).astype(F32)
    for j in range(experts):
        parts = []
        for p in range(inner):
            rank = meta[p][first + j : first + j + 1, :]
            goal = jnp.where(rank >= 0.0, rank + float(p * CAP), -1.0)
            parts.append(slot == goal)
        rows.append(parts)
    return rows


def experts_kernel(
    outer, inner, halves, chunks,
    resid, gain, routes, gates, length, keys, values, kgain, cosine, sine, owner, page_slot, wg, wu,
    act, metas, kv,
    rows, hidden, arrived, wbuf, pick, msend_buf, kvsend, kvrecv,
    send, recv, msend, mrecv, ksend, krecv, local, wsem,
):
    ep, core, z, y = place(outer, inner)
    peers = outer * inner
    tok, width = resid.shape
    cols = width // halves
    experts, _, ff = wg.shape
    slots = act.shape[2]
    piece = tok // chunks
    sib_kind = 1 + inner
    meta_rows = metas.shape[1]
    pages = owner.shape[1]
    kvw = keys.shape[1]

    def own_copy(h):
        return pltpu.make_async_copy(
            resid.at[:, pl.ds(h * cols, cols)], rows.at[ep, h], local.at[h]
        )

    def w_copy(j, which):
        return pltpu.make_async_copy(
            (wg, wu)[which].at[j], wbuf.at[j, :, pl.ds(which * ff, ff)], wsem.at[which, j]
        )

    for h in range(halves):
        own_copy(h).start()

    barrier = pltpu.get_barrier_semaphore()
    for k in range(1, peers):
        pl.semaphore_signal(
            barrier, inc=1, device_id={"ep": lax.rem(ep + k, peers), "section": core},
            device_id_type=MESH,
        )
    for k in range(1, halves):
        pl.semaphore_signal(
            barrier, inc=1, device_id={"ep": ep, "section": lax.rem(core + k, halves)},
            device_id_type=MESH,
        )
    for j in range(experts):
        for which in range(2):
            w_copy(j, which).start()
    for h in range(halves):
        own_copy(h).wait()
    pl.semaphore_wait(barrier, peers - 1 + halves - 1)

    def chunk_copy(block, half, k, kind, to_ep, to_core):
        at = (block, half, pl.ds(k * piece, piece), slice(None))
        return pltpu.make_async_remote_copy(
            src_ref=rows.at[at],
            dst_ref=rows.at[at],
            send_sem=send.at[kind, block],
            recv_sem=recv.at[block, half, k],
            device_id={"ep": to_ep, "section": to_core},
            device_id_type=MESH,
        )

    def block_sent(block, kind):
        pltpu.make_async_remote_copy(
            src_ref=rows.at[block, core],
            dst_ref=rows.at[block, core],
            send_sem=send.at[kind, block],
            recv_sem=recv.at[block, core, 0],
            device_id={"ep": ep, "section": lax.rem(core + 1, halves)},
            device_id_type=MESH,
        ).wait_send()

    def landed(block, half, k):
        chunk_copy(block, half, k, 0, ep, lax.rem(core + 1, halves)).wait_recv()

    def to_down(block, k):
        chunk_copy(block, core, k, 0, ep - inner, core).start()

    def to_up(block, k):
        chunk_copy(block, core, k, 1, ep + inner, core).start()

    def to_across(block, k):
        for n in range(1, inner):
            chunk_copy(block, core, k, 1 + n, z * inner + lax.rem(y + n, inner), core).start()

    def to_sibling(block, k):
        for n in range(1, halves):
            chunk_copy(
                block, core, k, sib_kind + n - 1, ep, lax.rem(core + n, halves)
            ).start()

    for k in range(chunks):
        pl.when(z > 0)(functools.partial(to_down, ep, k))
        pl.when(z < outer - 1)(functools.partial(to_up, ep, k))
        to_across(ep, k)

    number = experts * peers
    lane = lax.broadcasted_iota(jnp.int32, (1, tok), 1)
    live = lane.astype(F32) < length[...].astype(F32)
    mixing = gates[...] / jnp.sum(gates[...], axis=-1, keepdims=True)
    mixing = mixing.astype(BF16).astype(F32).T
    chosen = routes[...].astype(F32).T
    expert_id = lax.broadcasted_iota(jnp.int32, (number, tok), 0).astype(F32)
    hits = jnp.zeros((number, tok), F32)
    weight = jnp.zeros((number, tok), F32)
    for k in range(chosen.shape[0]):
        same = (chosen[k : k + 1, :] == expert_id) & live
        hits = hits + jnp.where(same, 1.0, 0.0)
        weight = weight + jnp.where(same, mixing[k : k + 1, :], 0.0)
    row_id = lax.broadcasted_iota(jnp.int32, (tok, tok), 0)
    col_id = lax.broadcasted_iota(jnp.int32, (tok, tok), 1)
    earlier = jnp.where(row_id < col_id, 1.0, 0.0).astype(BF16)
    rank = jnp.dot(hits.astype(BF16), earlier, preferred_element_type=F32)
    rank = jnp.where(hits > 0.0, rank, -1.0)

    own_t = jnp.zeros((1, tok), F32)
    slot_t = jnp.zeros((1, tok), F32)
    page_t = lax.div(lane, PAGE)
    for j in range(pages):
        own_t = jnp.where(page_t == j, owner[:, j : j + 1].astype(F32), own_t)
        slot_t = jnp.where(page_t == j, page_slot[:, j : j + 1].astype(F32), slot_t)
    own_here = jnp.broadcast_to(own_t, (tok, tok))
    before = (own_here.T == own_here) & (lax.div(row_id, PAGE) < lax.div(col_id, PAGE))
    order = jnp.sum(jnp.where(before, 1.0, 0.0), axis=0, keepdims=True) * (1.0 / PAGE)
    in_page = (lane - page_t * PAGE).astype(F32)
    key_t = (own_t * PER_OWNER + order) * PAGE + in_page
    goal_t = slot_t * PAGE + in_page
    pad_rows = jnp.zeros((meta_rows - 2 * experts - 2, tok), F32)
    for d in range(peers):
        mine = slice(d * experts, (d + 1) * experts)
        msend_buf[d] = jnp.concatenate([rank[mine], weight[mine], key_t, goal_t, pad_rows], axis=0)

    def meta_copy(n):
        to = lax.rem(ep + n, peers)
        return pltpu.make_async_remote_copy(
            src_ref=msend_buf.at[to],
            dst_ref=metas.at[ep],
            send_sem=msend.at[to],
            recv_sem=mrecv.at[ep],
            device_id={"ep": to, "section": core},
            device_id_type=MESH,
        )

    def kv_copy(n):
        to = lax.rem(ep + n, peers)
        return pltpu.make_async_remote_copy(
            src_ref=kvsend.at[to],
            dst_ref=kvrecv.at[ep],
            send_sem=ksend.at[to],
            recv_sem=krecv.at[ep],
            device_id={"ep": to, "section": core},
            device_id_type=MESH,
        )

    def from_peer(make, buf, sem, n):
        source = lax.rem(ep + n, peers)
        return pltpu.make_async_remote_copy(
            src_ref=buf.at[source],
            dst_ref=buf.at[source],
            send_sem=sem.at[source],
            recv_sem=make.at[source],
            device_id={"ep": source, "section": core},
            device_id_type=MESH,
        )

    for n in range(1, peers):
        meta_copy(n).start()
    metas[ep] = msend_buf[ep]

    live_c = lax.broadcasted_iota(jnp.int32, (tok, 1), 0).astype(F32) < length[...].astype(F32)
    head = kgain.shape[1]
    turned = []
    for h in range(kvw // head):
        x = keys[:, h * head : (h + 1) * head].astype(F32)
        x = x * lax.rsqrt(jnp.mean(x * x, axis=-1, keepdims=True) + 1e-06) * kgain[...].astype(F32)
        swapped = pltpu.roll(x, head // 2, 1)
        x = x * cosine[...] + swapped * sine[...]
        turned.append(jnp.where(live_c, x, 0.0).astype(BF16))
    turned.append(jnp.where(live_c, values[...].astype(F32), 0.0).astype(BF16))
    pairs = jnp.concatenate(turned, axis=1)
    piece_rows = PER_OWNER * PAGE
    group = 1
    while group * piece_rows < 256 and peers % (2 * group) == 0:
        group *= 2
    for d in range(0, peers, group):
        n = group * piece_rows
        want = (lax.broadcasted_iota(jnp.int32, (n, tok), 0) + d * piece_rows).astype(F32)
        chosen_rows = jnp.where(want == key_t, 1.0, 0.0).astype(BF16)
        out = jnp.dot(chosen_rows, pairs, preferred_element_type=F32).astype(BF16)
        for g in range(group):
            kvsend[d + g] = out[g * piece_rows : (g + 1) * piece_rows]
    for n in range(1, peers):
        kv_copy(n).start()
    kvrecv[ep] = kvsend[ep]

    def step(d):
        def body(k, carry):
            def one(side, zz):
                block = zz * inner + y
                landed(block, core, k)
                if side == 1:
                    pl.when(z > 0)(lambda: to_down(block, k))
                else:
                    pl.when(z < outer - 1)(lambda: to_up(block, k))
                to_across(block, k)
                to_sibling(block, k)

            sides(outer, z, d, one)
            return carry

        lax.fori_loop(0, chunks, body, 0)

    def across(zz):
        def body(k, carry):
            for n in range(1, inner):
                block = zz * inner + lax.rem(y + n, inner)
                landed(block, core, k)
                to_sibling(block, k)
            return carry

        lax.fori_loop(0, chunks, body, 0)

    tile = 512 if width % 512 == 0 else 128
    sub = 16

    def normalize(p, block):
        def body(i, carry):
            at = pl.ds(pl.multiple_of(i * sub, sub), sub)
            total = jnp.zeros((sub, 1), F32)
            for h in range(halves):
                for c in range(0, cols, tile):
                    x = rows[block, h, at, c : c + tile].astype(F32)
                    total = total + jnp.sum(x * x, axis=-1, keepdims=True)
            scale = lax.rsqrt(total * (1.0 / width) + 1e-06)
            to = pl.ds(pl.multiple_of(p * tok + i * sub, sub), sub)
            for h in range(halves):
                for c in range(0, cols, tile):
                    x = rows[block, h, at, c : c + tile].astype(F32)
                    g = gain[:, h * cols + c : h * cols + c + tile].astype(F32)
                    hidden[to, h * cols + c : h * cols + c + tile] = (x * scale * g).astype(BF16)
            return carry

        lax.fori_loop(0, tok // sub, body, 0)

    def compute(zz, own):
        for p in range(inner):
            block = zz * inner + p

            def wait_rest(block=block):
                for h in range(1, halves):
                    for k in range(chunks):
                        landed(block, lax.rem(core + h, halves), k)
                from_peer(mrecv, metas, msend, block - ep + peers).wait_recv()

            if own:
                pl.when(block != ep)(wait_rest)
            else:
                wait_rest()
            normalize(p, block)
        meta = [metas[zz * inner + p] for p in range(inner)]
        match = slot_match(meta, 0, experts, slots, inner)
        for j in range(experts):
            for p in range(inner):
                pick[j * slots : (j + 1) * slots, p * tok : (p + 1) * tok] = jnp.where(
                    match[j][p], 1.0, 0.0
                ).astype(BF16)

        def select(i, carry):
            at = pl.ds(pl.multiple_of(i * tile, tile), tile)
            arrived[:, at] = jnp.dot(
                pick[...], hidden[:, at], preferred_element_type=F32
            ).astype(BF16)
            return carry

        lax.fori_loop(0, width // tile, select, 0)

        def expert(j, carry):
            rows_j = pl.ds(pl.multiple_of(j * slots, slots), slots)
            both = jnp.dot(arrived[rows_j, :], wbuf[j], preferred_element_type=F32)
            gate = both[:, :ff]
            act[zz, j] = (gate * jax.nn.sigmoid(gate) * both[:, ff:]).astype(BF16)
            return carry

        lax.fori_loop(0, experts, expert, 0)

    step(1)
    across(z)
    for j in range(experts):
        for which in range(2):
            w_copy(j, which).wait()
    compute(z, True)

    def visit(i, carry):
        pl.when(i + 1 < outer)(lambda: step(i + 1))
        zz = near_column(outer, z, i)
        across(zz)
        compute(zz, False)
        return carry

    def place_pages():
        total = jnp.zeros((pages * PAGE, 2 * kvw), F32)
        for n in range(peers):
            if n:
                from_peer(krecv, kvrecv, ksend, n).wait_recv()
            source = lax.rem(ep + n, peers)
            meta = metas[source]
            key = meta[2 * experts : 2 * experts + 1, :]
            goal = meta[2 * experts + 1 : 2 * experts + 2, :]
            want = (lax.broadcasted_iota(jnp.int32, (piece_rows, tok), 0) + ep * piece_rows).astype(F32)
            spread = jnp.where(want == key, 1.0, 0.0).astype(BF16)
            slot = lax.broadcasted_iota(jnp.int32, (pages * PAGE, tok), 0).astype(F32)
            goals = jnp.where(slot == goal, 1.0, 0.0).astype(BF16)
            where = nt_dot(goals, spread).astype(BF16)
            total = total + jnp.dot(where, kvrecv[source], preferred_element_type=F32)
        kv[...] = total.astype(BF16)

    lax.fori_loop(1, outer, visit, 0)
    place_pages()

    def drain(block, carry):
        zz = lax.div(block, inner)
        same = lax.rem(block, inner) == y
        pl.when(same & (z > 0) & (zz >= z))(lambda: block_sent(block, 0))
        pl.when(same & (z < outer - 1) & (zz <= z))(lambda: block_sent(block, 1))
        for n in range(1, inner):
            pl.when(same)(functools.partial(block_sent, block, 1 + n))
        for n in range(1, halves):
            pl.when(block != ep)(functools.partial(block_sent, block, sib_kind + n - 1))
        return carry

    lax.fori_loop(0, peers, drain, 0)
    for n in range(1, peers):
        meta_copy(n).wait_send()
        kv_copy(n).wait_send()


def run_experts(outer, inner, halves, resid, gain, routes, gates, length, keys, values, kgain, cosine, sine, owner, page_slot, wg, wu):
    peers = outer * inner
    tok, width = resid.shape
    cols = width // halves
    experts, _, ff = wg.shape
    slots = -(-inner * CAP // 16) * 16
    meta_rows = -(-(2 * experts + 2) // 8) * 8
    chunks = 4 if peers <= 8 else 2
    kinds = 1 + inner + halves - 1
    kvw = keys.shape[1]
    pages = owner.shape[1]
    dma = pltpu.SemaphoreType.DMA
    vmem = pl.BlockSpec(memory_space=pltpu.VMEM)
    hbm = pl.BlockSpec(memory_space=pl.ANY)
    return pl.pallas_call(
        functools.partial(experts_kernel, outer, inner, halves, chunks),
        out_shape=(
            jax.ShapeDtypeStruct((outer, experts, slots, ff), BF16),
            jax.ShapeDtypeStruct((peers, meta_rows, tok), F32),
            jax.ShapeDtypeStruct((pages * PAGE, 2 * kvw), BF16),
        ),
        in_specs=[hbm] + [vmem] * 11 + [hbm, hbm],
        out_specs=(vmem, vmem, vmem),
        scratch_shapes=[
            pltpu.VMEM((peers, halves, tok, cols), BF16),
            pltpu.VMEM((inner * tok, width), BF16),
            pltpu.VMEM((experts * slots, width), BF16),
            pltpu.VMEM((experts, width, 2 * ff), BF16),
            pltpu.VMEM((experts * slots, inner * tok), BF16),
            pltpu.VMEM((peers, meta_rows, tok), F32),
            pltpu.VMEM((peers, PER_OWNER * PAGE, 2 * kvw), BF16),
            pltpu.VMEM((peers, PER_OWNER * PAGE, 2 * kvw), BF16),
            dma((kinds, peers)),
            dma((peers, halves, chunks)),
            dma((peers,)),
            dma((peers,)),
            dma((peers,)),
            dma((peers,)),
            dma((halves,)),
            dma((2, experts)),
        ],
        compiler_params=pltpu.CompilerParams(
            collective_id=0, has_side_effects=True, vmem_limit_bytes=LIMIT
        ),
        name="run_experts",
    )(resid, gain, routes, gates, length, keys, values, kgain, cosine, sine, owner, page_slot, wg, wu)


def scatter_kernel(
    outer, inner, halves, chunks,
    act, metas, wd, out,
    wbuf, part, pick, sbuf, acc, sib, yb, zb,
    wsem, ssend, srecv, ysend, yrecv, zsend, zrecv,
):
    ep, core, z, y = place(outer, inner)
    other = halves - 1 - core
    tok, cols = out.shape
    experts, ff, width = wd.shape
    slots = act.shape[2]
    piece = tok // chunks
    tile = 512 if cols % 512 == 0 else 128

    def w_copy(j):
        return pltpu.make_async_copy(wd.at[j], wbuf.at[j], wsem.at[j])

    for j in range(experts):
        w_copy(j).start()
    barrier = pltpu.get_barrier_semaphore()

    def signal(to_ep, to_core):
        pl.semaphore_signal(
            barrier, inc=1, device_id={"ep": to_ep, "section": to_core}, device_id_type=MESH
        )

    pl.when(z > 0)(lambda: signal(ep - inner, core))
    pl.when(z < outer - 1)(lambda: signal(ep + inner, core))
    for k in range(1, inner):
        signal(z * inner + lax.rem(y + k, inner), core)
    signal(ep, other)

    def sib_copy(block, slot=0):
        return pltpu.make_async_remote_copy(
            src_ref=sbuf.at[slot],
            dst_ref=sib.at[block],
            send_sem=ssend.at[block],
            recv_sem=srecv.at[block],
            device_id={"ep": ep, "section": other},
            device_id_type=MESH,
        )

    def y_copy(zz, n, k):
        to_y = lax.rem(y + n, inner)
        at = pl.ds(k * piece, piece)
        return pltpu.make_async_remote_copy(
            src_ref=acc.at[zz * inner + to_y, at],
            dst_ref=yb.at[n - 1, zz, at],
            send_sem=ysend.at[n - 1, zz, k],
            recv_sem=yrecv.at[n - 1, zz, k],
            device_id={"ep": z * inner + to_y, "section": core},
            device_id_type=MESH,
        )

    def z_copy(zz, slot, to_ep, k):
        at = pl.ds(k * piece, piece)
        return pltpu.make_async_remote_copy(
            src_ref=acc.at[zz * inner + y, at],
            dst_ref=zb.at[slot, at],
            send_sem=zsend.at[zz, k],
            recv_sem=zrecv.at[slot, k],
            device_id={"ep": to_ep, "section": core},
            device_id_type=MESH,
        )

    def add(dst, k, *sources):
        def body(i, carry):
            at = pl.ds(pl.multiple_of(k * piece + i * 16, 16), 16)
            for c in range(0, cols, tile):
                span = slice(c, c + tile)
                total = sources[0][at, span].astype(F32)
                for source in sources[1:]:
                    total = total + source[at, span].astype(F32)
                dst[at, span] = total.astype(dst.dtype)
            return carry

        lax.fori_loop(0, piece // 16, body, 0)

    def down(zz):
        def expert(j, carry):
            rows_j = pl.ds(pl.multiple_of(j * slots, slots), slots)

            def span(i, carry):
                at = pl.ds(pl.multiple_of(i * tile, tile), tile)
                part[rows_j, at] = jnp.dot(
                    act[zz, j], wbuf[j, :, at], preferred_element_type=F32
                ).astype(BF16)
                return carry

            return lax.fori_loop(0, width // tile, span, carry)

        lax.fori_loop(0, experts, expert, 0)

    def mix(zz, slot):
        meta = [metas[zz * inner + p] for p in range(inner)]
        match = slot_match(meta, 0, experts, slots, inner)
        for p in range(inner):
            weights = [
                jnp.where(match[j][p], meta[p][experts + j : experts + j + 1, :], 0.0)
                for j in range(experts)
            ]
            pick[p * tok : (p + 1) * tok, :] = jnp.concatenate(weights, axis=0).T.astype(BF16)

        def span(half, to_sib):
            def body(i, carry):
                at = pl.ds(pl.multiple_of(half * cols + i * tile, tile), tile)
                to = pl.ds(pl.multiple_of(i * tile, tile), tile)
                mixed = jnp.dot(pick[...], part[:, at], preferred_element_type=F32).astype(BF16)
                for p in range(inner):
                    piece_p = mixed[p * tok : (p + 1) * tok]
                    if to_sib:
                        sbuf[slot + p, :, to] = piece_p
                    else:
                        acc[zz * inner + p, :, to] = piece_p
                return carry

            lax.fori_loop(0, cols // tile, body, 0)

        span(other, True)
        for p in range(inner):
            sib_copy(zz * inner + p, slot + p).start()
        span(core, False)

    def hand_across(zz):
        for n in range(1, inner):
            block = zz * inner + lax.rem(y + n, inner)
            sib_copy(block).wait_recv()
            for k in range(chunks):
                add(acc.at[block], k, acc.at[block], sib.at[block])
                y_copy(zz, n, k).start()

    for j in range(experts):
        w_copy(j).wait()

    def far(i):
        return near_column(outer, z, outer - 1 - i)

    def visit(i, carry):
        zz = far(i)
        slot = lax.rem(i, 2) * inner
        down(zz)

        @pl.when(i == 0)
        def _():
            ends = jnp.where(z > 0, 1, 0) + jnp.where(z < outer - 1, 1, 0)
            pl.semaphore_wait(barrier, ends + inner - 1 + 1)

        @pl.when(i >= 2)
        def _():
            for p in range(inner):
                sib_copy(far(i - 2) * inner + p, slot + p).wait_send()

        mix(zz, slot)
        hand_across(zz)
        return carry

    lax.fori_loop(0, outer, visit, 0)

    def z_step(d, side, zz):
        block = zz * inner + y
        sib_copy(block).wait_recv()
        for k in range(chunks):
            for n in range(1, inner):
                y_copy(zz, n, k).wait_recv()
            parts = [acc.at[block], sib.at[block]] + [yb.at[n, zz] for n in range(inner - 1)]
            feeds = (z - side >= 0) & (z - side < outer)
            first = (d == 1) & (side == -1)
            slot = jnp.where(first, outer, zz)

            @pl.when(feeds)
            def _():
                z_copy(zz, zz, ep, k).wait_recv()
                add(acc.at[block], k, *parts, zb.at[zz])

            @pl.when(jnp.logical_not(feeds))
            def _():
                add(acc.at[block], k, *parts)

            z_copy(zz, slot, ep + side * inner, k).start()

    def last_step():
        block = ep
        sib_copy(block).wait_recv()
        for k in range(chunks):
            for n in range(1, inner):
                y_copy(z, n, k).wait_recv()
            parts = [acc.at[block], sib.at[block]] + [yb.at[n, z] for n in range(inner - 1)]

            @pl.when(z > 0)
            def _():
                z_copy(z, z, ep, k).wait_recv()

            @pl.when(z < outer - 1)
            def _():
                z_copy(z, outer, ep, k).wait_recv()

            @pl.when((z > 0) & (z < outer - 1))
            def _():
                add(out, k, *parts, zb.at[z], zb.at[outer])

            @pl.when((z == 0) & (z < outer - 1))
            def _():
                add(out, k, *parts, zb.at[outer])

            @pl.when((z > 0) & (z == outer - 1))
            def _():
                add(out, k, *parts, zb.at[z])

    def chain(i, carry):
        d = outer - 1 - i
        sides(outer, z, d, functools.partial(z_step, d))
        return carry

    lax.fori_loop(0, outer - 1, chain, 0)
    last_step()

    def close(i, carry):
        d = outer - 1 - i

        def one(side, zz):
            for k in range(chunks):
                z_copy(zz, zz, ep, k).wait_send()

        sides(outer, z, d, one)
        return carry

    lax.fori_loop(0, outer - 1, close, 0)

    def close_across(zz, carry):
        for n in range(1, inner):
            for k in range(chunks):
                y_copy(zz, n, k).wait_send()
        return carry

    lax.fori_loop(0, outer, close_across, 0)
    for i in range(max(0, outer - 2), outer):
        for p in range(inner):
            sib_copy(far(i) * inner + p, (i % 2) * inner + p).wait_send()


def scatter_sums(outer, inner, halves, act, metas, wd):
    peers = outer * inner
    tok = metas.shape[2]
    experts, ff, width = wd.shape
    slots = act.shape[2]
    shape = (tok, width // halves)
    chunks = 4 if peers <= 8 else 2
    dma = pltpu.SemaphoreType.DMA
    across = max(inner - 1, 1)
    lines = outer if inner > 1 else 1
    vmem = pl.BlockSpec(memory_space=pltpu.VMEM)
    return pl.pallas_call(
        functools.partial(scatter_kernel, outer, inner, halves, chunks),
        out_shape=jax.ShapeDtypeStruct(shape, BF16),
        in_specs=[vmem, vmem, pl.BlockSpec(memory_space=pl.ANY)],
        out_specs=vmem,
        scratch_shapes=[
            pltpu.VMEM((experts, ff, width), BF16),
            pltpu.VMEM((experts * slots, width), BF16),
            pltpu.VMEM((inner * tok, experts * slots), BF16),
            pltpu.VMEM((2 * inner,) + shape, BF16),
            pltpu.VMEM((peers,) + shape, BF16),
            pltpu.VMEM((peers,) + shape, BF16),
            pltpu.VMEM((across, lines) + shape, BF16),
            pltpu.VMEM((outer + 1,) + shape, BF16),
            dma((experts,)),
            dma((peers,)),
            dma((peers,)),
            dma((across, outer, chunks)),
            dma((across, outer, chunks)),
            dma((outer, chunks)),
            dma((outer + 1, chunks)),
        ],
        compiler_params=pltpu.CompilerParams(
            collective_id=1, has_side_effects=True, vmem_limit_bytes=LIMIT
        ),
        name="scatter_sums",
    )(act, metas, wd)


def layer_kernel(
    outer, inner, halves, chunks,
    resid, gain, routes, gates, length, keys, values, kgain, cosine, sine, owner, page_slot, wg, wu, wd,
    out, kv,
    rows, sib, yb, zb, xb, arrived, wbuf, dbuf, act, pick, comb, scale, metas, msend_buf, kvsend, kvrecv,
    send, recv, msend, mrecv, ksend, krecv, local, wsem, dsem, ssend, srecv, ysend, yrecv, zsend, zrecv, xsend, xrecv,
):
    ep, core, z, y = place(outer, inner)
    other = halves - 1 - core
    peers = outer * inner
    tok, width = resid.shape
    cols = width // halves
    experts, _, ff = wg.shape
    slots = act.shape[2]
    piece = tok // chunks
    sib_kind = 1 + inner
    meta_rows = metas.shape[1]
    pages = owner.shape[1]
    kvw = keys.shape[1]
    tile = 512 if cols % 512 == 0 else 128
    even = balanced(outer, inner)
    low = chunks // 2
    if even:
        mate = z + 1 - 2 * lax.rem(z, 2)
        skip = jnp.where(lax.rem(z, 2) == 0, outer - 1, 0)
        mate_skip = outer - 1 - skip
        is_end = (z == 0) | (z == outer - 1)
        columns = [z, mate, lax.rem(z + 2, outer), outer - 1 - z]
    else:
        columns = [near_column(outer, z, i) for i in range(outer)]

    def remote(src, dst, send_sem, recv_sem, to_ep, to_core):
        return pltpu.make_async_remote_copy(
            src_ref=src, dst_ref=dst, send_sem=send_sem, recv_sem=recv_sem,
            device_id={"ep": to_ep, "section": to_core}, device_id_type=MESH,
        )

    def own_copy(h):
        return pltpu.make_async_copy(
            resid.at[:, pl.ds(h * cols, cols)], rows.at[ep, h], local.at[h]
        )

    def w_copy(j, which):
        return pltpu.make_async_copy(
            (wg, wu)[which].at[j], wbuf.at[j, :, pl.ds(which * ff, ff)], wsem.at[which, j]
        )

    def d_copy(j):
        return pltpu.make_async_copy(wd.at[j], dbuf.at[j], dsem.at[j])

    for h in range(halves):
        own_copy(h).start()
    barrier = pltpu.get_barrier_semaphore()

    def greet(to_ep, to_core):
        pl.semaphore_signal(
            barrier, inc=1, device_id={"ep": to_ep, "section": to_core}, device_id_type=MESH
        )

    for k in range(1, peers):
        greet(lax.rem(ep + k, peers), core)
    greet(ep, other)
    for j in range(experts):
        for which in range(2):
            w_copy(j, which).start()
    for j in range(experts):
        d_copy(j).start()
    for h in range(halves):
        own_copy(h).wait()
    pl.semaphore_wait(barrier, peers - 1 + 1)

    def chunk_copy(block, half, k, kind, to_ep, to_core):
        at = (block, half, pl.ds(pl.multiple_of(k * piece, piece), piece), slice(None))
        return remote(
            rows.at[at], rows.at[at], send.at[kind, block], recv.at[block, half, k], to_ep, to_core
        )

    def block_sent(block, kind, amount=chunks):
        whole = rows.at[block, core, pl.ds(0, amount * piece)]
        remote(whole, whole, send.at[kind, block], recv.at[block, core, 0], ep, other).wait_send()

    def landed(block, half, k):
        chunk_copy(block, half, k, 0, ep, other).wait_recv()

    def to_down(block, k):
        chunk_copy(block, core, k, 0, ep - inner, core).start()

    def to_up(block, k):
        chunk_copy(block, core, k, 1, ep + inner, core).start()

    def to_across(block, k):
        for n in range(1, inner):
            chunk_copy(block, core, k, 1 + n, z * inner + lax.rem(y + n, inner), core).start()

    def to_sibling(block, k):
        chunk_copy(block, core, k, sib_kind, ep, other).start()

    for k in range(chunks):
        pl.when(z > 0)(functools.partial(to_down, ep, k))
        pl.when(z < outer - 1)(functools.partial(to_up, ep, k))
        to_across(ep, k)

    number = experts * peers
    lane = lax.broadcasted_iota(jnp.int32, (1, tok), 1)
    live = lane.astype(F32) < length[...].astype(F32)
    mixing = gates[...] / jnp.sum(gates[...], axis=0, keepdims=True)
    mixing = mixing.astype(BF16).astype(F32)
    chosen = routes[...].astype(F32)
    expert_id = lax.broadcasted_iota(jnp.int32, (number, tok), 0).astype(F32)
    hits = jnp.zeros((number, tok), F32)
    weight = jnp.zeros((number, tok), F32)
    for k in range(chosen.shape[0]):
        same = (chosen[k : k + 1, :] == expert_id) & live
        hits = hits + jnp.where(same, 1.0, 0.0)
        weight = weight + jnp.where(same, mixing[k : k + 1, :], 0.0)
    row_id = lax.broadcasted_iota(jnp.int32, (tok, tok), 0)
    col_id = lax.broadcasted_iota(jnp.int32, (tok, tok), 1)
    earlier = jnp.where(row_id < col_id, 1.0, 0.0).astype(BF16)
    rank = jnp.dot(hits.astype(BF16), earlier, preferred_element_type=F32)
    rank = jnp.where(hits > 0.0, rank, -1.0)

    own_t = jnp.zeros((1, tok), F32)
    slot_t = jnp.zeros((1, tok), F32)
    page_t = lax.div(lane, PAGE)
    for j in range(pages):
        own_t = jnp.where(page_t == j, owner[:, j : j + 1].astype(F32), own_t)
        slot_t = jnp.where(page_t == j, page_slot[:, j : j + 1].astype(F32), slot_t)
    own_here = jnp.broadcast_to(own_t, (tok, tok))
    before = (own_here.T == own_here) & (lax.div(row_id, PAGE) < lax.div(col_id, PAGE))
    order = jnp.sum(jnp.where(before, 1.0, 0.0), axis=0, keepdims=True) * (1.0 / PAGE)
    in_page = (lane - page_t * PAGE).astype(F32)
    key_t = (own_t * PER_OWNER + order) * PAGE + in_page
    goal_t = slot_t * PAGE + in_page
    pad_rows = jnp.zeros((meta_rows - 2 * experts - 2, tok), F32)
    for d in range(peers):
        mine = slice(d * experts, (d + 1) * experts)
        msend_buf[d] = jnp.concatenate([rank[mine], weight[mine], key_t, goal_t, pad_rows], axis=0)

    def meta_copy(n):
        to = lax.rem(ep + n, peers)
        return remote(msend_buf.at[to], metas.at[ep], msend.at[to], mrecv.at[ep], to, core)

    def kv_copy(n):
        to = lax.rem(ep + n, peers)
        return remote(kvsend.at[to], kvrecv.at[ep], ksend.at[to], krecv.at[ep], to, core)

    def meta_landed(block):
        remote(
            metas.at[block], metas.at[block], msend.at[block], mrecv.at[block], block, core
        ).wait_recv()

    def kv_landed(block):
        remote(
            kvrecv.at[block], kvrecv.at[block], ksend.at[block], krecv.at[block], block, core
        ).wait_recv()

    for n in range(1, peers):
        meta_copy(n).start()
    metas[ep] = msend_buf[ep]

    piece_rows = PER_OWNER * PAGE

    def prepare_pages():
        live_c = lax.broadcasted_iota(jnp.int32, (tok, 1), 0).astype(F32) < length[...].astype(F32)
        head = kgain.shape[1]
        turned = []
        for h in range(kvw // head):
            x = keys[:, h * head : (h + 1) * head].astype(F32)
            mean_square = jnp.mean(x * x, axis=-1, keepdims=True)
            x = x * lax.rsqrt(mean_square + 1e-06) * kgain[...].astype(F32)
            swapped = pltpu.roll(x, head // 2, 1)
            x = x * cosine[...] + swapped * sine[...]
            turned.append(jnp.where(live_c, x, 0.0).astype(BF16))
        turned.append(jnp.where(live_c, values[...].astype(F32), 0.0).astype(BF16))
        pairs = jnp.concatenate(turned, axis=1)
        group = 1
        while group * piece_rows < 256 and peers % (2 * group) == 0:
            group *= 2
        for d in range(0, peers, group):
            n = group * piece_rows
            want = (lax.broadcasted_iota(jnp.int32, (n, tok), 0) + d * piece_rows).astype(F32)
            chosen_rows = jnp.where(want == key_t, 1.0, 0.0).astype(BF16)
            picked = jnp.dot(chosen_rows, pairs, preferred_element_type=F32).astype(BF16)
            for g in range(group):
                kvsend[d + g] = picked[g * piece_rows : (g + 1) * piece_rows]
        kvrecv[ep] = kvsend[ep]

    def place_pages():
        total = jnp.zeros((pages * PAGE, 2 * kvw), F32)
        for n in range(peers):
            source = lax.rem(ep + n, peers)
            if n:
                kv_landed(source)
            meta = metas[source]
            key = meta[2 * experts : 2 * experts + 1, :]
            goal = meta[2 * experts + 1 : 2 * experts + 2, :]
            want = (lax.broadcasted_iota(jnp.int32, (piece_rows, tok), 0) + ep * piece_rows).astype(F32)
            spread = jnp.where(want == key, 1.0, 0.0).astype(BF16)
            slot = lax.broadcasted_iota(jnp.int32, (pages * PAGE, tok), 0).astype(F32)
            goals = jnp.where(slot == goal, 1.0, 0.0).astype(BF16)
            where = nt_dot(goals, spread).astype(BF16)
            total = total + jnp.dot(where, kvrecv[source], preferred_element_type=F32)
        kv[...] = total.astype(BF16)

    def step(d, first=0, last=chunks):
        def body(k, carry):
            def one(side, zz):
                block = zz * inner + y
                landed(block, core, k)
                if side == 1:
                    pl.when(z > 0)(lambda: to_down(block, k))
                else:
                    pl.when(z < outer - 1)(lambda: to_up(block, k))
                if even:
                    late = jnp.logical_not(is_end) & (zz == columns[3])
                    pl.when(jnp.logical_not(late | ((zz == skip) & (k >= low))))(
                        lambda: to_across(block, k)
                    )
                else:
                    to_across(block, k)
                to_sibling(block, k)

            sides(outer, z, d, one)
            return carry

        lax.fori_loop(first, last, body, 0)
        if even and d == 2:

            @pl.when(jnp.logical_not(is_end))
            def _():
                for k in range(chunks):
                    to_across(columns[3] * inner + y, k)

    def across(zz):
        def body(k, carry):
            for n in range(1, inner):
                block = zz * inner + lax.rem(y + n, inner)
                landed(block, core, k)
                to_sibling(block, k)
                if even:
                    around = (zz == mate_skip) & (k >= low)
                    pl.when(around & (mate < z))(lambda: to_down(block, k))
                    pl.when(around & (mate > z))(lambda: to_up(block, k))
            return carry

        lax.fori_loop(0, chunks, body, 0)

    sub = 16

    def row_scales(block, p, k):
        for i in range(piece // sub):
            at = pl.ds(pl.multiple_of(k * piece + i * sub, sub), sub)
            total = jnp.zeros((sub, tile), F32)
            for h in range(halves):
                for c in range(0, cols, tile):
                    x = rows[block, h, at, c : c + tile].astype(F32)
                    total = total + x * x
            mean_square = jnp.sum(total, axis=-1, keepdims=True) * (1.0 / width)
            to = pl.ds(pl.multiple_of(p * tok + k * piece + i * sub, sub), sub)
            scale[to, :] = jnp.broadcast_to(lax.rsqrt(mean_square + 1e-06), (sub, 128))

    def other_half(block, p, own):
        def body(k, carry):
            if own:
                pl.when(block != ep)(lambda: landed(block, other, k))
            else:
                landed(block, other, k)
            row_scales(block, p, k)
            return carry

        lax.fori_loop(0, chunks, body, 0)

    def matches(zz):
        meta = [metas[zz * inner + p] for p in range(inner)]
        return meta, slot_match(meta, 0, experts, slots, inner)

    def choose(zz):
        match = matches(zz)[1]
        for j in range(experts):
            for p in range(inner):
                pick[j * slots : (j + 1) * slots, p * tok : (p + 1) * tok] = jnp.where(
                    match[j][p], 1.0, 0.0
                ).astype(BF16)

    def weigh(zz):
        meta, match = matches(zz)
        for p in range(inner):
            weights = [
                jnp.where(match[j][p], meta[p][experts + j : experts + j + 1, :], 0.0)
                for j in range(experts)
            ]
            comb[p * tok : (p + 1) * tok, :] = jnp.concatenate(weights, axis=0).T.astype(BF16)

    def prepare(i):
        for p in range(inner):
            block = columns[i] * inner + p
            if i == 0:
                pl.when(block != ep)(functools.partial(meta_landed, block))
            else:
                meta_landed(block)
        choose(columns[i])
        if even and i > 0:
            weigh(columns[i])

    def hidden_layer(zz, own):
        for n in range(inner):
            p = lax.rem(y + n, inner)
            block = zz * inner + p
            other_half(block, p, own and n == 0)
        meta = [metas[zz * inner + p] for p in range(inner)]
        match = slot_match(meta, 0, experts, slots, inner)
        factors = []
        lanes = [
            scale[p * tok : (p + 1) * tok, :tok].T[0:1, :] for p in range(inner)
        ]
        for j in range(experts):
            factor = jnp.zeros((slots, 1), F32)
            for p in range(inner):
                factor = factor + jnp.sum(
                    jnp.where(match[j][p], lanes[p], 0.0), axis=-1, keepdims=True
                )
            factors.append(factor)
        factor = jnp.concatenate(factors, axis=0)
        span = min(cols, SELECT)
        for h in range(halves):
            def select(i, carry, h=h):
                at = pl.ds(pl.multiple_of(i * span, span), span)
                to = pl.ds(pl.multiple_of(h * cols + i * span, span), span)
                source = rows[pl.ds(zz * inner, inner), h, :, at].reshape(inner * tok, span)
                found = jnp.dot(pick[...], source, preferred_element_type=F32)
                arrived[:, to] = (found * factor * gain[to].astype(F32)[None, :]).astype(BF16)
                return carry

            lax.fori_loop(0, cols // span, select, 0)

        def expert(j, carry):
            rows_j = pl.ds(pl.multiple_of(j * slots, slots), slots)
            both = jnp.dot(arrived[rows_j, :], wbuf[j], preferred_element_type=F32)
            gate = both[:, :ff]
            act[zz, j] = (gate * jax.nn.sigmoid(gate) * both[:, ff:]).astype(BF16)
            return carry

        lax.fori_loop(0, experts, expert, 0)

    def sib_copy(block):
        return remote(rows.at[block, other], sib.at[block], ssend.at[block], srecv.at[block], ep, other)

    def y_copy(zz, n, k):
        to_y = lax.rem(y + n, inner)
        at = pl.ds(pl.multiple_of(k * piece, piece), piece)
        return remote(
            rows.at[zz * inner + to_y, core, at], yb.at[n - 1, zz, at],
            ysend.at[n - 1, zz, k], yrecv.at[n - 1, zz, k], z * inner + to_y, core,
        )

    def x_copy(k):
        at = pl.ds(pl.multiple_of(k * piece, piece), piece)
        return remote(
            rows.at[mate * inner + lax.rem(y + 1, inner), core, at], xb.at[at],
            xsend.at[k], xrecv.at[k], mate * inner + y, core,
        )

    def z_copy(zz, slot, to_ep, k):
        at = pl.ds(pl.multiple_of(k * piece, piece), piece)
        return remote(
            rows.at[zz * inner + y, core, at], zb.at[slot, at],
            zsend.at[zz, k], zrecv.at[slot, k], to_ep, core,
        )

    def add(dst, k, *sources):
        def body(i, carry):
            at = pl.ds(pl.multiple_of(k * piece + i * 16, 16), 16)
            for c in range(0, cols, tile):
                part = slice(c, c + tile)
                total = sources[0][at, part].astype(F32)
                for source in sources[1:]:
                    total = total + source[at, part].astype(F32)
                dst[at, part] = total.astype(dst.dtype)
            return carry

        lax.fori_loop(0, piece // 16, body, 0)

    def output_layer(zz):
        for p in range(inner):
            block = zz * inner + p
            same = y == p
            pl.when(same & (z > 0) & (zz >= z))(functools.partial(block_sent, block, 0))
            pl.when(same & (z < outer - 1) & (zz <= z))(functools.partial(block_sent, block, 1))
            for n in range(1, inner):
                if even:
                    pl.when(same & (zz != skip))(functools.partial(block_sent, block, 1 + n))
                    pl.when(same & (zz == skip))(functools.partial(block_sent, block, 1 + n, low))
                else:
                    pl.when(same)(functools.partial(block_sent, block, 1 + n))
            if even:
                around = (y != p) & (zz == mate_skip)
                rest = chunks - low
                pl.when(around & (mate < z))(functools.partial(block_sent, block, 0, rest))
                pl.when(around & (mate > z))(functools.partial(block_sent, block, 1, rest))
            pl.when(block != ep)(functools.partial(block_sent, block, sib_kind))
        def half_of(half, to_sib):
            at = pl.ds(pl.multiple_of(half * cols, cols), cols)

            def expert(j, carry):
                rows_j = pl.ds(pl.multiple_of(j * slots, slots), slots)
                arrived[rows_j, at] = jnp.dot(
                    act[zz, j], dbuf[j, :, at], preferred_element_type=F32
                ).astype(BF16)
                return carry

            lax.fori_loop(0, experts, expert, 0, unroll=True)
            span = min(cols, MIX)

            def body(i, carry):
                at = pl.ds(pl.multiple_of(half * cols + i * span, span), span)
                to = pl.ds(pl.multiple_of(i * span, span), span)
                mixed = jnp.dot(comb[...], arrived[:, at], preferred_element_type=F32).astype(BF16)
                for p in range(inner):
                    rows[zz * inner + p, half, :, to] = mixed[p * tok : (p + 1) * tok]
                return carry

            lax.fori_loop(0, cols // span, body, 0)
            if to_sib:
                for p in range(inner):
                    sib_copy(zz * inner + p).start()

        half_of(other, True)
        half_of(core, False)

    def hand_across(zz, how="y"):
        for n in range(1, inner):
            block = zz * inner + lax.rem(y + n, inner)
            mine = rows.at[block, core]
            sib_copy(block).wait_recv()

            def body(k, carry):
                if how == "merge":
                    x_copy(k).wait_recv()
                    add(mine, k, mine, sib.at[block], xb)
                else:
                    add(mine, k, mine, sib.at[block])
                if how == "x":
                    x_copy(k).start()
                else:
                    y_copy(zz, n, k).start()
                return carry

            lax.fori_loop(0, chunks, body, 0)

    def z_step(*targets):
        for zz in targets:
            sib_copy(zz * inner + y).wait_recv()

        def one(zz, k):
            block = zz * inner + y
            mine = rows.at[block, core]
            up = zz > z
            feeds = jnp.where(up, z > 0, z < outer - 1)
            ends = jnp.logical_not(feeds)
            ahead = jnp.where(up, z + 1, z - 1)
            slot = jnp.where((ahead == zz) & (zz < z), outer, zz)
            with_y = zz != mate if even else zz != z
            without = jnp.logical_not(with_y)
            others = [yb.at[n, zz] for n in range(inner - 1)]

            @pl.when(with_y)
            def _():
                for n in range(1, inner):
                    y_copy(zz, n, k).wait_recv()

            pl.when(feeds)(lambda: z_copy(zz, zz, ep, k).wait_recv())
            pl.when(feeds & with_y)(lambda: add(mine, k, mine, sib.at[block], *others, zb.at[zz]))
            pl.when(ends & with_y)(lambda: add(mine, k, mine, sib.at[block], *others))
            pl.when(feeds & without)(lambda: add(mine, k, mine, sib.at[block], zb.at[zz]))
            pl.when(ends & without)(lambda: add(mine, k, mine, sib.at[block]))
            z_copy(zz, slot, ahead * inner + y, k).start()

        def body(k, carry):
            for zz in targets:
                one(zz, k)
            return carry

        lax.fori_loop(0, chunks, body, 0)

    def last_step():
        sib_copy(ep).wait_recv()
        for k in range(chunks):
            for n in range(1, inner):
                y_copy(z, n, k).wait_recv()
            parts = [rows.at[ep, core], sib.at[ep]] + [yb.at[n, z] for n in range(inner - 1)]
            pl.when(z > 0)(lambda: z_copy(z, z, ep, k).wait_recv())
            pl.when(z < outer - 1)(lambda: z_copy(z, outer, ep, k).wait_recv())
            pl.when((z > 0) & (z < outer - 1))(
                lambda: add(out, k, *parts, zb.at[z], zb.at[outer])
            )
            pl.when((z == 0) & (z < outer - 1))(lambda: add(out, k, *parts, zb.at[outer]))
            pl.when((z > 0) & (z == outer - 1))(lambda: add(out, k, *parts, zb.at[z]))

    prepare_pages()
    def send_pages():
        for n in range(1, peers):
            kv_copy(n).start()

    def wait_weights(i):
        if i == 0:
            for j in range(experts):
                for which in range(2):
                    w_copy(j, which).wait()

    middle = jnp.logical_not(is_end) if even else None
    for i in range(outer):
        if i + 1 < outer and not (even and i == 2):
            step(i + 1)
        if even and i == 2:

            @pl.when(is_end)
            def _():
                step(3, low)
                across(columns[2])

        prepare(i)
        if not (even and i == 2):
            across(columns[i])
        if i == outer - 1:
            send_pages()
        wait_weights(i)
        hidden_layer(columns[i], i == 0)
        if i == 0:
            for j in range(experts):
                d_copy(j).wait()
        if even and i == 1:
            pl.when(is_end)(lambda: step(3, 0, low))
            pl.when(middle)(lambda: across(columns[2]))
            output_layer(mate)

            @pl.when(is_end)
            def _():
                hand_across(mate, "x")
                z_step(mate)
        elif even and i > 1:
            output_layer(columns[i])
            hand_across(columns[i])
            if i == 2:
                pl.when(middle)(lambda: hand_across(mate, "x"))
        elif not even and i >= outer - 2:
            weigh(columns[i])
            output_layer(columns[i])
            hand_across(columns[i])
    if even:
        weigh(columns[0])
        pl.when(is_end)(lambda: z_step(columns[2]))
        output_layer(columns[0])
        hand_across(columns[0], "merge")
        pl.when(is_end)(lambda: z_step(columns[3]))

        @pl.when(middle)
        def _():
            z_step(columns[2])
            z_step(mate, columns[3])

        place_pages()
    else:
        for i in range(outer - 3, -1, -1):
            weigh(columns[i])
            output_layer(columns[i])
            hand_across(columns[i])
        for d in range(outer - 1, 0, -1):
            sides(outer, z, d, lambda side, zz: z_step(zz))
        place_pages()
    last_step()

    def y_sent(zz, n, k):
        y_copy(zz, n, k).wait_send()

    for d in range(outer - 1, 0, -1):
        def sent(side, zz):
            for k in range(chunks):
                z_copy(zz, zz, ep, k).wait_send()

        sides(outer, z, d, sent)
    for zz in range(outer):
        for n in range(1, inner):
            for k in range(chunks):
                if even:
                    pl.when(mate != zz)(functools.partial(y_sent, zz, n, k))
                else:
                    y_sent(zz, n, k)
    if even:
        for k in range(chunks):
            x_copy(k).wait_send()
    for block in range(peers):
        sib_copy(block).wait_send()
    for n in range(1, peers):
        meta_copy(n).wait_send()
        kv_copy(n).wait_send()


def balanced(outer, inner):
    return outer == 4 and inner == 2


def run_layer(outer, inner, halves, resid, gain, routes, gates, length, keys, values, kgain, cosine, sine, owner, page_slot, wg, wu, wd):
    peers = outer * inner
    tok, width = resid.shape
    cols = width // halves
    experts, _, ff = wg.shape
    slots = -(-inner * CAP // 16) * 16
    meta_rows = -(-(2 * experts + 2) // 8) * 8
    chunks = CHUNKS
    kinds = 1 + inner + halves - 1
    kvw = keys.shape[1]
    pages = owner.shape[1]
    across = max(inner - 1, 1)
    lines = outer if inner > 1 else 1
    dma = pltpu.SemaphoreType.DMA
    vmem = pl.BlockSpec(memory_space=pltpu.VMEM)
    hbm = pl.BlockSpec(memory_space=pl.ANY)
    return pl.pallas_call(
        functools.partial(layer_kernel, outer, inner, halves, chunks),
        out_shape=(
            jax.ShapeDtypeStruct((tok, cols), BF16),
            jax.ShapeDtypeStruct((pages * PAGE, 2 * kvw), BF16),
        ),
        in_specs=[hbm] + [vmem] * 11 + [hbm] * 3,
        out_specs=(vmem, vmem),
        scratch_shapes=[
            pltpu.VMEM((peers, halves, tok, cols), BF16),
            pltpu.VMEM((peers, tok, cols), BF16),
            pltpu.VMEM((across, lines, tok, cols), BF16),
            pltpu.VMEM((outer + 1, tok, cols), BF16),
            pltpu.VMEM((tok, cols) if balanced(outer, inner) else (16, 128), BF16),
            pltpu.VMEM((experts * slots, width), BF16),
            pltpu.VMEM((experts, width, 2 * ff), BF16),
            pltpu.VMEM((experts, ff, width), BF16),
            pltpu.VMEM((outer, experts, slots, ff), BF16),
            pltpu.VMEM((experts * slots, inner * tok), BF16),
            pltpu.VMEM((inner * tok, experts * slots), BF16),
            pltpu.VMEM((inner * tok, 128), F32),
            pltpu.VMEM((peers, meta_rows, tok), F32),
            pltpu.VMEM((peers, meta_rows, tok), F32),
            pltpu.VMEM((peers, PER_OWNER * PAGE, 2 * kvw), BF16),
            pltpu.VMEM((peers, PER_OWNER * PAGE, 2 * kvw), BF16),
            dma((kinds, peers)),
            dma((peers, halves, chunks)),
            dma((peers,)),
            dma((peers,)),
            dma((peers,)),
            dma((peers,)),
            dma((halves,)),
            dma((2, experts)),
            dma((experts,)),
            dma((peers,)),
            dma((peers,)),
            dma((across, outer, chunks)),
            dma((across, outer, chunks)),
            dma((outer, chunks)),
            dma((outer + 1, chunks)),
            dma((chunks,)),
            dma((chunks,)),
        ],
        compiler_params=pltpu.CompilerParams(
            collective_id=0, has_side_effects=True, vmem_limit_bytes=LIMIT
        ),
        name="run_layer",
    )(resid, gain, routes, gates, length, keys, values, kgain, cosine, sine, owner, page_slot, wg, wu, wd)


def fits(outer, inner, halves, tok, width, experts, ff):
    peers = outer * inner
    block = tok * width // halves * 2
    rows = (halves * peers + peers + outer * (inner - 1) + outer + 1) * block
    return rows + 6 * experts * ff * width + 4 * experts * inner * CAP * width < LIMIT


def inner_size(mesh):
    try:
        line = mesh.devices[0, :, 0]
        coords = [tuple(device.coords) for device in line]
        inner = 1
        while inner < len(coords) and sum(a != b for a, b in zip(coords[inner], coords[0])) == 1:
            axis = [i for i in range(3) if coords[1][i] != coords[0][i]][0]
            if coords[inner][axis] == coords[0][axis]:
                break
            inner += 1
        return inner if inner < len(coords) and len(coords) % inner == 0 else 1
    except (AttributeError, IndexError, TypeError):
        return 1


def turns(tok, head):
    half = head // 2
    frequency = np.exp(np.arange(half) * (-2.0 / head) * math.log(1000000.0))
    angles = np.arange(tok)[:, None] * frequency
    cosine, sine = np.cos(angles), np.sin(angles)
    return (
        np.concatenate([cosine, cosine], axis=1).astype(np.float32),
        np.concatenate([-sine, sine], axis=1).astype(np.float32),
    )


def shards(
    inner,
    resid,
    norm_gain,
    gate_logits,
    routes,
    w_gate,
    w_up,
    w_down,
    keys_raw,
    values_raw,
    k_gain,
    lengths,
    page_owner,
    page_slot,
):
    halves = lax.axis_size("section")
    outer = lax.axis_size("ep") // inner
    cosine, sine = turns(resid.shape[0], k_gain.shape[0])
    tok, width = resid.shape
    if fits(outer, inner, halves, tok, width, w_gate.shape[0], w_gate.shape[2]):
        moe_out, kv = run_layer(
            outer, inner, halves,
            resid, norm_gain, routes.T, gate_logits.T, lengths[None, :],
            keys_raw, values_raw, k_gain[None, :], jnp.asarray(cosine), jnp.asarray(sine),
            page_owner, page_slot, w_gate, w_up, w_down,
        )
        return (moe_out, kv.reshape(page_owner.shape[1], PAGE, 2, keys_raw.shape[1]))
    act, metas, kv = run_experts(
        outer, inner, halves,
        resid, norm_gain[None, :], routes, gate_logits, lengths[None, :],
        keys_raw, values_raw, k_gain[None, :], jnp.asarray(cosine), jnp.asarray(sine),
        page_owner, page_slot, w_gate, w_up,
    )
    kv_cache = kv.reshape(page_owner.shape[1], PAGE, 2, keys_raw.shape[1])
    moe_out = scatter_sums(outer, inner, halves, act, metas, w_down)
    return (moe_out, kv_cache)


def solution(mesh):
    in_specs = (
        P(("groups", "ep"), None),
        P(),
        P(("groups", "ep"), None),
        P(("groups", "ep"), None),
        P("ep", None, "section"),
        P("ep", None, "section"),
        P("ep", "section", None),
        P(("groups", "ep"), "section"),
        P(("groups", "ep"), "section"),
        P(),
        P(("groups", "ep")),
        P(("groups", "ep"), None),
        P(("groups", "ep"), None),
    )
    out_specs = (P(("groups", "ep"), "section"), P(("groups", "ep"), None, None, "section"))
    body = functools.partial(shards, inner_size(mesh))
    return jax.shard_map(body, mesh=mesh, in_specs=in_specs, out_specs=out_specs, check_vma=False)
```
